256 devices in a mesh: cluster: 64 (over z, x, core), sub: 4 (over y).
Axes of the slice: x: 4, y: 4, z: 8, core: 2. Of those that a mesh axis runs over, the one named last changes fastest.
Arguments:
- mantissas: int32 [64, 64, 168, 128], P('cluster', 'sub'), may hold values from -128 to 127
- exponents: int32 [64, 64, 14], P('cluster', 'sub'), may hold values from -9 to -6
- channel: bfloat16 [64, 64, 2, 64, 128], P('cluster', 'sub'), may hold values from -0.5 to 0.5
- inverses: bfloat16 [64, 64, 2, 128, 128], P('cluster', 'sub'), may hold values from -4 to 4, as said below
Outputs:
- detected: bfloat16 [64, 168, 256], P('sub')
The draws below stay inside these ranges and needn't reach their ends.
Inputs may be any that keep to these rules, and one draw needn't show every extreme that they name: `inverses`: each real part has a positive diagonal; the matrices are otherwise dense.
All inputs are finite; a program needn't handle non-finite values.
Results may differ from the reference program's by a relative error of at most 0.0074.
Values may be sent and summed in bfloat16 or wider, within the bound.
No kernel may reach another device: no remote copies, remote signals or barrier semaphores. Data moves between devices by JAX's collectives and lax.ppermute only.
A program may use at most 64 MiB of HBM per device.

```python
import jax
import jax.numpy as jnp
from jax import lax

USER_COUNT = 128
CLUSTER_ANTENNAS = 64
BLOCK_TONES = 12
SLOT_SYMBOLS = 14
ITERS = 3
RESOURCE_BLOCKS = 64
ANTENNA_GROUPS = 64


def draw_inverses(key, part):
    first, second = jax.random.split(key, 2)
    shape = (ANTENNA_GROUPS, RESOURCE_BLOCKS, 2, USER_COUNT, USER_COUNT)
    noise = jax.random.normal(first, shape, jnp.float32) * 0.05
    diagonal = jax.random.uniform(second, (ANTENNA_GROUPS, RESOURCE_BLOCKS, 1, USER_COUNT, 1), jnp.float32, 0.5, 1.5)
    identity = jnp.eye(USER_COUNT, dtype=jnp.float32)
    realpart = (jnp.arange(2) == 0).astype(jnp.float32)[None, None, :, None, None]
    result = noise + diagonal * identity * realpart
    return result.astype(jnp.bfloat16)


def with_ends(drawn, rng, least, high):
    extent = drawn.shape
    spot = [jax.random.randint(jax.random.fold_in(rng, axis), (), 0, extent[axis]) for axis in range(len(extent))]
    drawn = drawn.at[tuple(spot)].set(least)
    longest = extent.index(max(extent))
    spot[longest] = (spot[longest] + 1) % extent[longest]
    return drawn.at[tuple(spot)].set(high)


def level_of(stream_key, extent, shards, least, largest):
    gain, own = 1.0, jax.random.fold_in(stream_key, 6)
    for position, blocks in shards:
        draws = jnp.exp(jax.random.uniform(jax.random.fold_in(own, position), (blocks,), jnp.float32, least / len(shards), largest / len(shards)))
        gain = gain * jnp.repeat(draws, extent[position] // blocks).reshape([-1 if axis == position else 1 for axis in range(len(extent))])
    return gain


def scatter_about(rng, dims, deviation, reach, cuts=(), held_as=jnp.bfloat16):
    values = deviation * jax.random.normal(rng, dims, jnp.float32)
    if cuts:
        values = values * level_of(rng, dims, cuts, -0.22, 0.18)
    return jnp.clip(values, -reach, reach).astype(held_as)


def setup_inputs(seed: int = 0) -> dict:
    splits = jax.random.split(jax.random.key(seed), 5)
    mantissas = with_ends(jax.random.randint(splits[0], (ANTENNA_GROUPS, RESOURCE_BLOCKS, SLOT_SYMBOLS * BLOCK_TONES, 2 * CLUSTER_ANTENNAS), -128, 128), jax.random.fold_in(splits[0], 1), -128, 127).astype(jnp.int32)
    exponents = with_ends(jax.random.randint(splits[1], (ANTENNA_GROUPS, RESOURCE_BLOCKS, SLOT_SYMBOLS), -9, -5), jax.random.fold_in(splits[1], 1), -9, (-5) - 1).astype(jnp.int32)
    channel = scatter_about(splits[2], (ANTENNA_GROUPS, RESOURCE_BLOCKS, 2, CLUSTER_ANTENNAS, USER_COUNT), (2 * CLUSTER_ANTENNAS) ** -0.5, 0.5, ((0, 64), (1, 4)))
    inverses = draw_inverses(jax.random.fold_in(splits[4], 71), 0)
    return dict(mantissas=mantissas, exponents=exponents, channel=channel, inverses=inverses)


RHO = 0.5

def complex_block(real, imag):
    top = jnp.concatenate([real, -imag], axis=-1)
    bottom = jnp.concatenate([imag, real], axis=-1)
    return jnp.concatenate([top, bottom], axis=-2)

def one_block(index, mantissas, exponents, channel, inverses):
    mant = lax.dynamic_index_in_dim(mantissas, index, 1, keepdims=False)
    expo = lax.dynamic_index_in_dim(exponents, index, 1, keepdims=False)
    chan = lax.dynamic_index_in_dim(channel, index, 1, keepdims=False)
    inv = lax.dynamic_index_in_dim(inverses, index, 1, keepdims=False)
    scale = jnp.repeat(jnp.exp2(expo.astype(jnp.float32)), BLOCK_TONES, axis=1)
    signal = (mant.astype(jnp.float32) * scale[:, :, None]).astype(jnp.bfloat16)
    match = complex_block(chan[:, 0], chan[:, 1])
    matched_filter = jnp.einsum('csa,cau->csu', signal.astype(jnp.float32), match.astype(jnp.float32))
    solve_block = complex_block(inv[:, 0], inv[:, 1]).astype(jnp.float32)
    consensus = jnp.zeros(matched_filter.shape[1:], jnp.float32)
    dual = jnp.zeros(matched_filter.shape, jnp.float32)
    for step in range(ITERS):
        rhs = (matched_filter + RHO * (consensus[None] - dual)).astype(jnp.bfloat16)
        local = jnp.einsum('csk,cjk->csj', rhs.astype(jnp.float32), solve_block)
        term = local + dual
        total = lax.optimization_barrier(jnp.sum(term, axis=0))
        consensus = (total / ANTENNA_GROUPS).astype(jnp.bfloat16).astype(jnp.float32)
        dual = term - consensus[None]
    return consensus.astype(jnp.bfloat16)

def reference(mantissas, exponents, channel, inverses):

    def per_block(index):
        return one_block(index, mantissas, exponents, channel, inverses)
    consensus = lax.map(per_block, jnp.arange(RESOURCE_BLOCKS, dtype=jnp.int32)).astype(jnp.float32)
    column_list = lax.optimization_barrier(jnp.sum(consensus * consensus, axis=(0, 1)))
    power = (column_list[:USER_COUNT] + column_list[USER_COUNT:]) / (RESOURCE_BLOCKS * SLOT_SYMBOLS * BLOCK_TONES)
    factor = lax.rsqrt(power + 1e-06)
    factor = jnp.concatenate([factor, factor])
    return (consensus * factor).astype(jnp.bfloat16)
```

```python
import jax
import jax.numpy as jnp
from jax import lax
from jax.experimental import pallas as pl
from jax.experimental.pallas import tpu as pltpu
from jax.sharding import PartitionSpec as P


Z, X, C = 8, 4, 2
CLUSTERS = Z * X * C
PART = 48
BF, F32 = jnp.bfloat16, jnp.float32


def place(z, x, c):
    return (z * X + x) * C + c


def shifted(dz=0, dx=0, dc=0):
    return [
        (place(z, x, c), place((z + dz) % Z, (x + dx) % X, c ^ dc))
        for z in range(Z)
        for x in range(X)
        for c in range(C)
    ]


def pair_shifted(dx, dp):
    return [
        (place(z, x, c), place(z ^ dp, (x + dx) % X, c))
        for z in range(Z)
        for x in range(X)
        for c in range(C)
    ]


Z_RINGS = [[place(z, x, c) for z in range(Z)] for x in range(X) for c in range(C)]
SLOTS = ((0, 0), (1, 0), (3, 0), (0, 1), (2, 0), (1, 1), (3, 1), (2, 1))


def moved(value, pairs):
    return lax.ppermute(value, "cluster", pairs)


def dot(a, b):
    return jnp.dot(a, b, preferred_element_type=F32)


def complex_square(x, y):
    top = jnp.concatenate([x, y], axis=1)
    return top, jnp.concatenate([top, jnp.concatenate([-y, x], axis=1)], axis=0)


def pack_kernel(here_ref, mant_ref, expo_ref, chan_ref, inv_ref, *outs):
    x, pair, c = here_ref[0], here_ref[1], here_ref[2]
    row = lax.broadcasted_iota(jnp.int32, (168, 14), 0)
    first = lax.broadcasted_iota(jnp.int32, (168, 14), 1) * 12
    inside = (row >= first) & (row < first + 12)
    for out, (dx, dp) in zip(outs, SLOTS):
        for k, side in enumerate((c, 1 - c)):
            r = side * 8 + lax.rem(x + dx, X) * 2 + (1 - pair if dp else pair)
            out[k, 0:256, :] = inv_ref[r]
            out[k, 256:384, :] = chan_ref[r]
            scale = jnp.exp2(expo_ref[pl.ds(r, 1), :].astype(F32))
            scale = jnp.sum(jnp.where(inside, scale, 0.0), axis=1, keepdims=True)
            out[k, 384:552, :] = (mant_ref[r].astype(F32) * scale).astype(BF)


def packed(here, mant, expo, chan, inv):
    vmem = pl.BlockSpec(memory_space=pltpu.VMEM)
    return pl.pallas_call(
        pack_kernel,
        in_specs=[pl.BlockSpec(memory_space=pltpu.SMEM)] + [vmem] * 4,
        out_specs=[vmem] * 8,
        out_shape=[jax.ShapeDtypeStruct((2, 552, 128), BF)] * 8,
        cost_estimate=pl.CostEstimate(flops=6000000, bytes_accessed=5000000, transcendentals=0),
    )(here, mant, expo, chan, inv)


def add_clusters(held, p1, p2, t, av):
    def one(raw):
        top, square = complex_square(raw[0:128, :].T, raw[128:256, :].T)
        cr, ci = raw[256:320, :], raw[320:384, :]
        match = jnp.concatenate(
            [jnp.concatenate([cr, -ci], axis=1), jnp.concatenate([ci, cr], axis=1)], axis=0
        )
        m = dot(raw[384:552, :], match).astype(BF)
        t1 = dot(m, square)
        t2 = dot(t1.astype(BF), square)
        t3 = dot(t2.astype(BF), square)
        return t1, t2, t3, top.astype(F32), dot(top, square)

    def two(k, carry):
        a, b = one(held[2 * k]), one(held[2 * k + 1])
        t1, t2, t3, top, second = (u + v for u, v in zip(a, b))
        p1[0:168, :] += t1
        p2[0:168, :] += t2 - 2.0 * t1
        t[0:168, :] += 3.0 * t1 - 1.5 * t2 + 0.25 * t3
        av[0:128, :] += top
        av[128:256, :] += second
        return carry

    lax.fori_loop(0, 4, two, 0)


def first_kernel(*refs):
    raws, (p1, p2, t, av), held = refs[:8], refs[8:12], refs[12]
    for k in range(8):
        held[k] = raws[k][0]
    for ref in (p1, p2, t, av):
        ref[...] = jnp.zeros_like(ref)
    add_clusters(held, p1, p2, t, av)


def second_kernel(q_ref, *refs):
    raws, before, outs = refs[:8], refs[8:12], refs[12:16]
    held, (p1, p2, t, av) = refs[16], refs[17:]
    for k in range(8):
        held[k] = raws[k][0]
    for ref, old in zip((p1, p2, t, av), before):
        ref[...] = old[...]
    add_clusters(held, p1, p2, t, av)
    ones = (
        lax.broadcasted_iota(jnp.int32, (128, 256), 0) == lax.broadcasted_iota(jnp.int32, (128, 256), 1)
    ).astype(F32) * 16.0
    first = av[0:128, :]
    av[0:128, :] = first - ones
    av[128:256, :] = av[128:256, :] - 2.0 * first + ones
    for d, out in enumerate(outs):
        q = lax.rem(q_ref[0] + d, 4)
        rows = pl.ds(pl.multiple_of(q * PART, PART), PART)
        out[0:48, :] = p1[rows, :].astype(BF)
        out[48:96, :] = p2[rows, :].astype(BF)
        out[96:144, :] = t[rows, :].astype(BF)
        out[144:208, :] = av[pl.ds(pl.multiple_of(q * 64, 64), 64), :].astype(BF)


SUMS = ((192, 256), (192, 256), (192, 256), (256, 256))


def cluster_specs():
    own = pl.BlockSpec((1, 552, 128), lambda i, *_: (0, 0, 0))
    other = pl.BlockSpec((1, 552, 128), lambda i, *_: (1, 0, 0))
    return [own] * 4 + [other] * 4


def first_partials(raws):
    full = [pl.BlockSpec(shape, lambda i: (0, 0)) for shape in SUMS]
    return pl.pallas_call(
        first_kernel,
        grid=(1,),
        in_specs=cluster_specs(),
        out_specs=full,
        out_shape=[jax.ShapeDtypeStruct(shape, F32) for shape in SUMS],
        scratch_shapes=[pltpu.VMEM((8, 552, 128), BF)],
        cost_estimate=pl.CostEstimate(flops=2000000000, bytes_accessed=3000000, transcendentals=0),
    )(*raws)


def second_partials(q, raws, before):
    full = [pl.BlockSpec(shape, lambda i, q: (0, 0)) for shape in SUMS]
    return pl.pallas_call(
        second_kernel,
        grid_spec=pltpu.PrefetchScalarGridSpec(
            num_scalar_prefetch=1,
            grid=(1,),
            in_specs=cluster_specs() + full,
            out_specs=[pl.BlockSpec((208, 256), lambda i, q: (0, 0))] * 4,
            scratch_shapes=[pltpu.VMEM((8, 552, 128), BF)] + [pltpu.VMEM(shape, F32) for shape in SUMS],
        ),
        out_shape=[jax.ShapeDtypeStruct((208, 256), BF)] * 4,
        cost_estimate=pl.CostEstimate(flops=2000000000, bytes_accessed=3000000, transcendentals=0),
    )(q, *raws, *before)


def total_kernel(*refs):
    parts, (p_ref, av_ref) = refs[:4], refs[4:]
    total = parts[0][...].astype(F32)
    for part in parts[1:]:
        total += part[...].astype(F32)
    total = total * (1.0 / CLUSTERS)
    p_ref[...] = total[0:144, :]
    av_ref[...] = total[144:208, :].astype(BF)


def totals(parts):
    return pl.pallas_call(
        total_kernel,
        out_shape=(
            jax.ShapeDtypeStruct((144, 256), F32),
            jax.ShapeDtypeStruct((64, 256), BF),
        ),
    )(*parts)


def dot_wide(a, b):
    high = a.astype(BF)
    low = (a - high.astype(F32)).astype(BF)
    return dot(high, b) + dot(low, b)


def solve_kernel(quarter_ref, p_ref, a0, a1, a2, a3, out_ref, av):
    for d, part in enumerate((a0, a1, a2, a3)):
        av[lax.rem(quarter_ref[0] + 4 - d, 4)] = part[...]
    mean = jnp.concatenate([av[0], av[1]], axis=0)
    second = jnp.concatenate([av[2], av[3]], axis=0)
    _, mean = complex_square(mean[:, 0:128], mean[:, 128:256])
    _, second = complex_square(second[:, 0:128], second[:, 128:256])
    z1, p2, t = p_ref[0:48, :], p_ref[48:96, :], p_ref[96:144, :]
    g = dot_wide(z1, mean)
    z3 = t + 1.5 * g - 0.5 * dot_wide(z1, second) + dot_wide(g - 0.5 * p2, mean)
    out_ref[...] = z3.astype(BF)


def solved(quarter, p, avs):
    vmem = pl.BlockSpec(memory_space=pltpu.VMEM)
    return pl.pallas_call(
        solve_kernel,
        in_specs=[pl.BlockSpec(memory_space=pltpu.SMEM)] + [vmem] * 5,
        out_specs=vmem,
        out_shape=jax.ShapeDtypeStruct((PART, 256), BF),
        scratch_shapes=[pltpu.VMEM((4, 64, 256), BF)],
    )(quarter, p, *avs)


def power_kernel(order_ref, *refs):
    parts, out_ref, rows = refs[:8], refs[8], refs[9]
    for k, part in enumerate(parts):
        value = part[...].astype(F32)
        rows[order_ref[k]] = jnp.sum(value * value, axis=(0, 1))[None, :]
    total = rows[0]
    for k in range(1, 8):
        total += rows[k]
    out_ref[...] = total[:, 0:128] + total[:, 128:256]


def power_of(order, parts):
    vmem = pl.BlockSpec(memory_space=pltpu.VMEM)
    return pl.pallas_call(
        power_kernel,
        in_specs=[pl.BlockSpec(memory_space=pltpu.SMEM)] + [vmem] * 8,
        out_specs=vmem,
        out_shape=jax.ShapeDtypeStruct((1, 128), F32),
        scratch_shapes=[pltpu.VMEM((8, 1, 256), F32)],
    )(order, *parts)


def finish_kernel(vectors, order_ref, power_ref, *refs):
    parts, out_ref = refs[:8], refs[8]
    power = power_ref[0] + power_ref[1] + power_ref[2] + power_ref[3]
    factor = lax.rsqrt(power * (1.0 / vectors) + 1e-06)
    factor = jnp.concatenate([factor, factor], axis=1)
    for k, part in enumerate(parts):
        for zz in range(Z):
            start = zz // 2 * PART
            size = min(168 - start, PART)
            value = part[zz, 0:size, :].astype(F32) * factor
            out_ref[order_ref[k], zz % 2, start : start + size, :] = value.astype(BF)


def finished(order, power, parts, vectors):
    vmem = pl.BlockSpec(memory_space=pltpu.VMEM)
    return pl.pallas_call(
        lambda *refs: finish_kernel(vectors, *refs),
        in_specs=[pl.BlockSpec(memory_space=pltpu.SMEM)] + [vmem] * 9,
        out_specs=vmem,
        out_shape=jax.ShapeDtypeStruct((8, 2, 168, 256), BF),
    )(order, power, *parts)


def per_device(mantissas, exponents, channel, inverses):
    place_here = lax.axis_index("cluster")
    c = place_here % C
    x = place_here // C % X
    z = place_here // (C * X)
    mant, expo = mantissas[0], exponents[0]
    blocks, vectors, _ = mant.shape
    here = jnp.stack([x, z % 2, c]).astype(jnp.int32)
    sent = packed(
        here, mant, expo, channel[0].reshape(blocks, 128, 128), inverses[0].reshape(blocks, 256, 128)
    )
    raws = [sent[0]]
    for k in range(1, 8):
        raws.append(moved(sent[k], pair_shifted(*SLOTS[k])))
    swapped = []
    for k in range(8):
        swapped.append(moved(raws[k], shifted(dc=1)))
    q = (z // 2).reshape(1).astype(jnp.int32)
    before = first_partials(raws[:4] + swapped[:4])
    sums = second_partials(q, raws[4:] + swapped[4:], before)
    parts = [sums[0]] + [moved(sums[d], shifted(dz=2 * d)) for d in (2, 1, 3)]
    p, av = totals(parts)
    avs = [av] + [moved(av, shifted(dz=2 * d)) for d in (1, 2, 3)]
    share = solved(q, p, avs)
    copies = jnp.broadcast_to(share, (Z, PART, 256))
    mine = lax.all_to_all(copies, "cluster", 0, 0, tiled=True, axis_index_groups=Z_RINGS)
    same = [mine] + [moved(mine, shifted(dx=d)) for d in (1, 2, 3)]
    other = [moved(value, shifted(dc=1)) for value in same]
    order = jnp.stack(
        [side * X + (x + X - d) % X for side in (c, 1 - c) for d in range(X)]
    ).astype(jnp.int32)
    power = power_of(order, same + other)
    power = lax.all_to_all(jnp.broadcast_to(power, (4, 1, 128)), "sub", 0, 0, tiled=True)
    total = blocks * lax.axis_size("sub") * vectors
    return finished(order, power, same + other, total).reshape(blocks, vectors, 256)


def solution(mesh):
    placed = (
        P("cluster", "sub", None, None),
        P("cluster", "sub", None),
        P("cluster", "sub", None, None, None),
        P("cluster", "sub", None, None, None),
    )
    return jax.shard_map(
        per_device, mesh=mesh, in_specs=placed, out_specs=P("sub", None, None), check_vma=False
    )
```

```python
import jax
import jax.numpy as jnp
from jax import lax
from jax.experimental import pallas as pl
from jax.experimental.pallas import tpu as pltpu
from jax.sharding import PartitionSpec as P


Z, X, C = 8, 4, 2
CLUSTERS = Z * X * C
ROWS = 42
PART = 48
EARLY = 6
BF, F32 = jnp.bfloat16, jnp.float32


def place(z, x, c):
    return (z * X + x) * C + c


def shifted(dz=0, dx=0, dc=0):
    return [
        (place(z, x, c), place((z + dz) % Z, (x + dx) % X, c ^ dc))
        for z in range(Z)
        for x in range(X)
        for c in range(C)
    ]


def pair_shifted(dx, dp):
    return [
        (place(z, x, c), place(z ^ dp, (x + dx) % X, c))
        for z in range(Z)
        for x in range(X)
        for c in range(C)
    ]


Z_RINGS = [[place(z, x, c) for z in range(Z)] for x in range(X) for c in range(C)]
SLOTS = ((0, 0), (1, 0), (3, 0), (0, 1), (2, 0), (1, 1), (3, 1), (2, 1))


def moved(value, pairs):
    return lax.ppermute(value, "cluster", pairs)


def dot(a, b):
    return jnp.dot(a, b, preferred_element_type=F32)


def complex_square(x, y):
    top = jnp.concatenate([x, y], axis=1)
    return top, jnp.concatenate([top, jnp.concatenate([-y, x], axis=1)], axis=0)


def pack_kernel(here_ref, mant_ref, expo_ref, chan_ref, inv_ref, *outs):
    x, pair, c = here_ref[0], here_ref[1], here_ref[2]
    row = lax.broadcasted_iota(jnp.int32, (168, 14), 0)
    first = lax.broadcasted_iota(jnp.int32, (168, 14), 1) * 12
    inside = ((row >= first) & (row < first + 12)).astype(F32).astype(BF)
    scales = dot(inside, jnp.exp2(expo_ref[...].astype(F32)).astype(BF))
    lane = lax.broadcasted_iota(jnp.int32, (168, 16), 1)
    for out, (dx, dp) in zip(outs, SLOTS):
        for k, side in enumerate((c, 1 - c)):
            r = side * 8 + lax.rem(x + dx, X) * 2 + (1 - pair if dp else pair)
            out[k, 0:256, :] = inv_ref[r]
            out[k, 256:384, :] = chan_ref[r]
            scale = jnp.sum(jnp.where(lane == r, scales, 0.0), axis=1, keepdims=True)
            out[k, 384:552, :] = (mant_ref[r].astype(F32) * scale).astype(BF)


def packed(here, mant, expo, chan, inv):
    vmem = pl.BlockSpec(memory_space=pltpu.VMEM)
    return pl.pallas_call(
        pack_kernel,
        in_specs=[pl.BlockSpec(memory_space=pltpu.SMEM)] + [vmem] * 4,
        out_specs=[vmem] * 8,
        out_shape=[jax.ShapeDtypeStruct((2, 552, 128), BF)] * 8,
        cost_estimate=pl.CostEstimate(flops=6000000, bytes_accessed=5000000, transcendentals=0),
    )(here, mant, expo, chan, inv)


def square_of(raw):
    return complex_square(raw[0:128, :].T, raw[128:256, :].T)


def add_means(raws, av):
    for raw in raws:
        top, square = square_of(raw)
        av[0:128, :] += top.astype(F32)
        av[128:256, :] += dot(top, square)


def add_estimates(raws, p, d, t, av=None):
    sums = None
    for raw in raws:
        top, square = square_of(raw)
        cr, ci = raw[256:320, :], raw[320:384, :]
        match = jnp.concatenate(
            [jnp.concatenate([cr, -ci], axis=1), jnp.concatenate([ci, cr], axis=1)], axis=0
        )
        m = dot(raw[384:552, :], match).astype(BF)
        t1 = dot(m, square)
        t2 = dot(t1.astype(BF), square)
        t3 = dot(t2.astype(BF), square)
        new = (t1, t2, t3) + ((top.astype(F32), dot(top, square)) if av is not None else ())
        sums = new if sums is None else tuple(u + v for u, v in zip(sums, new))
    t1, t2, t3 = sums[:3]
    p[0:168, :] += t1
    d[0:168, :] += t2 - 2.0 * t1
    t[0:168, :] += 3.0 * t1 - 1.5 * t2 + 0.25 * t3
    if av is not None:
        av[0:128, :] += sums[3]
        av[128:256, :] += sums[4]


def early_kernel(*refs):
    raws, (p, d, t, av), held = refs[: 2 * EARLY], refs[2 * EARLY : -1], refs[-1]
    for k, raw in enumerate(raws):
        held[k] = raw[0]
    for ref in (p, d, t, av):
        ref[...] = jnp.zeros_like(ref)

    def two(k, carry):
        add_estimates((held[2 * k], held[2 * k + 1]), p, d, t, av)
        return carry

    lax.fori_loop(0, EARLY, two, 0)


def mean_kernel(*refs):
    raws, before, out, av = refs[:-3], refs[-3], refs[-2], refs[-1]
    av[...] = before[...]
    add_means([raw[0, 0:256, :] for raw in raws], av)
    ones = (
        lax.broadcasted_iota(jnp.int32, (128, 256), 0) == lax.broadcasted_iota(jnp.int32, (128, 256), 1)
    ).astype(F32) * 16.0
    first = av[0:128, :]
    out[0:128, :] = (first - ones).astype(BF)
    out[128:256, :] = (av[128:256, :] - 2.0 * first + ones).astype(BF)


def late_kernel(q_ref, *refs):
    n = 2 * (8 - EARLY)
    raws, before, outs = refs[:n], refs[n : n + 3], refs[n + 3 : n + 7]
    sums, shares = refs[n + 7 : n + 10], refs[n + 10]
    for ref, old in zip(sums, before):
        ref[...] = old[...]
    for k in range(0, n, 2):
        add_estimates((raws[k][0], raws[k + 1][0]), *sums)
    shares[...] = jnp.zeros_like(shares)
    for k, ref in enumerate(sums):
        for part in range(4):
            shares[part, k * PART : k * PART + ROWS, :] = ref[part * ROWS : part * ROWS + ROWS, :]
    for away, out in enumerate(outs):
        out[...] = shares[lax.rem(q_ref[0] + away, 4)].astype(BF)


SUM = (168, 256)
SUMS = (SUM, SUM, SUM, (256, 256))
COST = pl.CostEstimate(flops=2000000000, bytes_accessed=3000000, transcendentals=0)


def cluster_specs(slots):
    own = pl.BlockSpec((1, 552, 128), lambda i, *_: (0, 0, 0))
    other = pl.BlockSpec((1, 552, 128), lambda i, *_: (1, 0, 0))
    return [own, other] * slots


def full(shape):
    return pl.BlockSpec(shape, lambda i, *_: (0,) * len(shape))


def early_sums(raws):
    return pl.pallas_call(
        early_kernel,
        grid=(1,),
        in_specs=cluster_specs(EARLY),
        out_specs=[full(shape) for shape in SUMS],
        out_shape=[jax.ShapeDtypeStruct(shape, F32) for shape in SUMS],
        scratch_shapes=[pltpu.VMEM((2 * EARLY, 552, 128), BF)],
        cost_estimate=COST,
    )(*raws)


def mean_sums(raws, before):
    return pl.pallas_call(
        mean_kernel,
        grid=(1,),
        in_specs=cluster_specs(8 - EARLY) + [full((256, 256))],
        out_specs=full((256, 256)),
        out_shape=jax.ShapeDtypeStruct((256, 256), BF),
        scratch_shapes=[pltpu.VMEM((256, 256), F32)],
        cost_estimate=COST,
    )(*raws, before)


def late_sums(q, raws, before):
    return pl.pallas_call(
        late_kernel,
        grid_spec=pltpu.PrefetchScalarGridSpec(
            num_scalar_prefetch=1,
            grid=(1,),
            in_specs=cluster_specs(8 - EARLY) + [full(SUM)] * 3,
            out_specs=[full((144, 256))] * 4,
            scratch_shapes=[pltpu.VMEM(SUM, F32)] * 3 + [pltpu.VMEM((4, 144, 256), F32)],
        ),
        out_shape=[jax.ShapeDtypeStruct((144, 256), BF)] * 4,
        cost_estimate=COST,
    )(q, *raws, *before)


def dot_wide(a, b):
    high = a.astype(BF)
    low = (a - high.astype(F32)).astype(BF)
    return dot(high, b) + dot(low, b)


def mean_of(parts):
    total = parts[0][...].astype(F32)
    for part in parts[1:]:
        total += part[...].astype(F32)
    return total * (1.0 / CLUSTERS)


def solve_kernel(*refs):
    sums, means, share_ref, power_ref = refs[:4], refs[4:8], refs[8], refs[9]
    total, mean = mean_of(sums), mean_of(means).astype(BF)
    _, first = complex_square(mean[0:128, 0:128], mean[0:128, 128:256])
    _, second = complex_square(mean[128:256, 0:128], mean[128:256, 128:256])
    z1, d, t = total[0:48, :], total[48:96, :], total[96:144, :]
    g = dot_wide(z1, first)
    z3 = t + 1.5 * g - 0.5 * dot_wide(z1, second) + dot_wide(g - 0.5 * d, first)
    share_ref[...] = z3.astype(BF)
    kept = z3.astype(BF).astype(F32)
    power = jnp.sum(kept * kept, axis=0, keepdims=True)
    power_ref[...] = power[:, 0:128] + power[:, 128:256]


def whole(kernel, ins, outs, scratch=()):
    vmem = pl.BlockSpec(memory_space=pltpu.VMEM)
    return pl.pallas_call(
        kernel,
        in_specs=[
            pl.BlockSpec(memory_space=pltpu.SMEM) if value.dtype == jnp.int32 else vmem for value in ins
        ],
        out_specs=jax.tree.map(lambda _: vmem, outs),
        out_shape=outs,
        scratch_shapes=scratch,
    )(*ins)


def solved(sums, means):
    outs = (jax.ShapeDtypeStruct((PART, 256), BF), jax.ShapeDtypeStruct((1, 128), F32))
    return whole(solve_kernel, (*sums, *means), outs)


def copies_kernel(share_ref, p0, p1, p2, p3, out_ref):
    power = p0[...] + p1[...] + p2[...] + p3[...]
    value = share_ref[...].astype(F32)
    row = lax.broadcasted_iota(jnp.int32, (PART, 256), 0)
    for k in range(3):
        term = power.astype(BF).astype(F32)
        power = power - term
        wide = jnp.concatenate([term, jnp.zeros_like(term)], axis=1)
        value = jnp.where(row == ROWS + k, wide, value)
    value = value.astype(BF)
    for k in range(Z):
        out_ref[k] = value


def finish_kernel(vectors, order_ref, *refs):
    parts, out_ref, rows, block = refs[:8], refs[8], refs[9], refs[10]
    for k, part in enumerate(parts):
        power = jnp.zeros((1, 256), F32)
        for zz in range(Z):
            tail = part[zz, 40:48, :].astype(F32)
            power += tail[2:3, :] + tail[3:4, :] + tail[4:5, :]
        rows[order_ref[k]] = power[:, 0:128]
    power = rows[0]
    for k in range(1, 8):
        power += rows[k]
    factor = lax.rsqrt(power * (1.0 / vectors) + 1e-06)
    factor = jnp.concatenate([factor, factor], axis=1)
    for k, part in enumerate(parts):
        for pair in range(2):
            for q in range(4):
                value = part[2 * q + pair].astype(F32) * factor
                block[pair, q * ROWS : q * ROWS + ROWS, :] = value[0:ROWS, :]
            out_ref[order_ref[k], pair] = block[pair].astype(BF)


def finished(order, parts, vectors):
    return whole(
        lambda *refs: finish_kernel(vectors, *refs),
        (order, *parts),
        jax.ShapeDtypeStruct((8, 2, 168, 256), BF),
        (pltpu.VMEM((8, 1, 128), F32), pltpu.VMEM((2, 168, 256), F32)),
    )


def per_device(mantissas, exponents, channel, inverses):
    place_here = lax.axis_index("cluster")
    c = place_here % C
    x = place_here // C % X
    z = place_here // (C * X)
    mant, expo = mantissas[0], exponents[0].T
    blocks, vectors, _ = mant.shape
    here = jnp.stack([x, z % 2, c]).astype(jnp.int32)
    sent = packed(
        here, mant, expo, channel[0].reshape(blocks, 128, 128), inverses[0].reshape(blocks, 256, 128)
    )
    raws = [sent[0]]
    for k in range(1, 8):
        raws.append(moved(sent[k], pair_shifted(*SLOTS[k])))
    swapped = []
    for k in range(8):
        swapped.append(moved(raws[k], shifted(dc=1)))
    q = (z // 2).reshape(1).astype(jnp.int32)
    slots = [part for pair in zip(raws, swapped) for part in pair]
    before = early_sums(slots[: 2 * EARLY])
    means = mean_sums(slots[2 * EARLY :], before[3])
    means = [means, means, means, means]
    for d in (2, 1, 3):
        means[d] = moved(means[0], shifted(dz=2 * d))
    sums = late_sums(q, slots[2 * EARLY :], before[:3])
    sums = [sums[0]] + [moved(sums[d], shifted(dz=2 * d)) for d in (2, 1, 3)]
    share, power = solved(sums, means)
    powers = [power] + [
        lax.ppermute(power, "sub", [(y, (y + d) % 4) for y in range(4)]) for d in (2, 1, 3)
    ]
    copies = whole(copies_kernel, (share, *powers), jax.ShapeDtypeStruct((Z, PART, 256), BF))
    mine = lax.all_to_all(copies, "cluster", 0, 0, tiled=True, axis_index_groups=Z_RINGS)
    same = [mine] + [moved(mine, shifted(dx=d)) for d in (1, 2, 3)]
    other = [moved(value, shifted(dc=1)) for value in same]
    order = jnp.stack(
        [side * X + (x + X - d) % X for side in (c, 1 - c) for d in range(X)]
    ).astype(jnp.int32)
    total = blocks * lax.axis_size("sub") * vectors
    return finished(order, same + other, total).reshape(blocks, vectors, 256)


def solution(mesh):
    placed = (
        P("cluster", "sub", None, None),
        P("cluster", "sub", None),
        P("cluster", "sub", None, None, None),
        P("cluster", "sub", None, None, None),
    )
    return jax.shard_map(
        per_device, mesh=mesh, in_specs=placed, out_specs=P("sub", None, None), check_vma=False
    )
```

```python
import jax
import jax.numpy as jnp
from jax import lax
from jax.experimental import pallas as pl
from jax.experimental.pallas import tpu as pltpu
from jax.sharding import PartitionSpec as P


Z, X, C = 8, 4, 2
CLUSTERS = Z * X * C
ROWS = 176
EARLY = 6
BF, F32 = jnp.bfloat16, jnp.float32


def place(z, x, c):
    return (z * X + x) * C + c


def shifted(dz=0, dx=0, dc=0):
    return [
        (place(z, x, c), place((z + dz) % Z, (x + dx) % X, c ^ dc))
        for z in range(Z)
        for x in range(X)
        for c in range(C)
    ]


def pair_shifted(dx, dp):
    return [
        (place(z, x, c), place(z ^ dp, (x + dx) % X, c))
        for z in range(Z)
        for x in range(X)
        for c in range(C)
    ]


SLOTS = ((0, 0), (1, 0), (3, 0), (0, 1), (2, 0), (1, 1), (3, 1), (2, 1))


def moved(value, pairs):
    return lax.ppermute(value, "cluster", pairs)


def dot(a, b):
    return jnp.dot(a, b, preferred_element_type=F32)


def complex_square(x, y):
    top = jnp.concatenate([x, y], axis=1)
    return top, jnp.concatenate([top, jnp.concatenate([-y, x], axis=1)], axis=0)


def pack_kernel(x_ref, pair_ref, c_ref, mant_ref, expo_ref, chan_ref, inv_ref, *outs):
    x, pair, c = x_ref[0], pair_ref[0], c_ref[0]
    row = lax.broadcasted_iota(jnp.int32, (168, 14), 0)
    first = lax.broadcasted_iota(jnp.int32, (168, 14), 1) * 12
    inside = ((row >= first) & (row < first + 12)).astype(F32).astype(BF)
    expo = jnp.concatenate([expo_ref[t] for t in range(14)], axis=0)
    scales = dot(inside, jnp.exp2(expo.astype(F32)).astype(BF))
    lane = lax.broadcasted_iota(jnp.int32, (168, 16), 1)
    for out, (dx, dp) in zip(outs, SLOTS):
        for k, side in enumerate((c, 1 - c)):
            r = side * 8 + lax.rem(x + dx, X) * 2 + (1 - pair if dp else pair)
            out[k, 0:256, :] = inv_ref[r]
            out[k, 256:384, :] = chan_ref[r]
            scale = jnp.sum(jnp.where(lane == r, scales, 0.0), axis=1, keepdims=True)
            out[k, 384:552, :] = (mant_ref[r].astype(F32) * scale).astype(BF)


def whole(kernel, ins, outs, scratch=(), cost=None):
    vmem = pl.BlockSpec(memory_space=pltpu.VMEM)
    return pl.pallas_call(
        kernel,
        in_specs=[pl.BlockSpec(memory_space=pltpu.SMEM) if value.shape == (1,) else vmem for value in ins],
        out_specs=jax.tree.map(lambda _: vmem, outs),
        out_shape=outs,
        scratch_shapes=scratch,
        cost_estimate=cost,
    )(*ins)


def packed(*ins):
    cost = pl.CostEstimate(flops=6000000, bytes_accessed=5000000, transcendentals=0)
    return whole(pack_kernel, ins, [jax.ShapeDtypeStruct((2, 552, 128), BF)] * 8, cost=cost)


def square_of(raw):
    return complex_square(raw[0:128, :].T, raw[128:256, :].T)


def add_means(raws, av):
    for raw in raws:
        top, square = square_of(raw)
        av[0:128, :] += top.astype(F32)
        av[128:256, :] += dot(top, square)


def add_estimates(raws, p, d, t, av=None):
    sums = None
    for raw in raws:
        top, square = square_of(raw)
        cr, ci = raw[256:320, :], raw[320:384, :]
        match = jnp.concatenate(
            [jnp.concatenate([cr, -ci], axis=1), jnp.concatenate([ci, cr], axis=1)], axis=0
        )
        m = dot(raw[384:552, :], match).astype(BF)
        t1 = dot(m, square)
        t2 = dot(t1.astype(BF), square)
        t3 = dot(t2.astype(BF), square)
        new = (t1, t2, t3) + ((top.astype(F32), dot(top, square)) if av is not None else ())
        sums = new if sums is None else tuple(u + v for u, v in zip(sums, new))
    t1, t2, t3 = sums[:3]
    p[0:168, :] += t1
    d[0:168, :] += t2 - 2.0 * t1
    t[0:168, :] += 3.0 * t1 - 1.5 * t2 + 0.25 * t3
    if av is not None:
        av[0:128, :] += sums[3]
        av[128:256, :] += sums[4]


def early_kernel(*refs):
    raws, (p, d, t, av), held = refs[: 2 * EARLY], refs[2 * EARLY : -1], refs[-1]
    for k, raw in enumerate(raws):
        held[k] = raw[0]
    for ref in (p, d, t, av):
        ref[...] = jnp.zeros_like(ref)

    def two(k, carry):
        add_estimates((held[2 * k], held[2 * k + 1]), p, d, t, av)
        return carry

    lax.fori_loop(0, EARLY, two, 0)


def mean_kernel(*refs):
    raws, before, out, av = refs[:-3], refs[-3], refs[-2], refs[-1]
    av[...] = before[...]
    add_means([raw[0, 0:256, :] for raw in raws], av)
    ones = (
        lax.broadcasted_iota(jnp.int32, (128, 256), 0) == lax.broadcasted_iota(jnp.int32, (128, 256), 1)
    ).astype(F32) * 16.0
    first = av[0:128, :]
    out[0:128, :] = (first - ones).astype(BF)
    out[128:256, :] = (av[128:256, :] - 2.0 * first + ones).astype(BF)


def late_kernel(*refs):
    n = 2 * (8 - EARLY)
    raws, before, sums = refs[:n], refs[n : n + 3], refs[n + 3 :]
    for ref, old in zip(sums, before):
        ref[...] = old[...]
    for k in range(0, n, 2):
        add_estimates((raws[k][0], raws[k + 1][0]), *sums)


SUM = (168, 256)
SUMS = (SUM, SUM, SUM, (256, 256))
COST = pl.CostEstimate(flops=2000000000, bytes_accessed=3000000, transcendentals=0)


def cluster_specs(slots):
    own = pl.BlockSpec((1, 552, 128), lambda i, *_: (0, 0, 0))
    other = pl.BlockSpec((1, 552, 128), lambda i, *_: (1, 0, 0))
    return [own, other] * slots


def full(shape):
    return pl.BlockSpec(shape, lambda i, *_: (0,) * len(shape))


def early_sums(raws):
    return pl.pallas_call(
        early_kernel,
        grid=(1,),
        in_specs=cluster_specs(EARLY),
        out_specs=[full(shape) for shape in SUMS],
        out_shape=[jax.ShapeDtypeStruct(shape, F32) for shape in SUMS],
        scratch_shapes=[pltpu.VMEM((2 * EARLY, 552, 128), BF)],
        cost_estimate=COST,
    )(*raws)


def mean_sums(raws, before):
    return pl.pallas_call(
        mean_kernel,
        grid=(1,),
        in_specs=cluster_specs(8 - EARLY) + [full((256, 256))],
        out_specs=full((256, 256)),
        out_shape=jax.ShapeDtypeStruct((256, 256), BF),
        scratch_shapes=[pltpu.VMEM((256, 256), F32)],
        cost_estimate=COST,
    )(*raws, before)


def late_sums(raws, before):
    return pl.pallas_call(
        late_kernel,
        grid=(1,),
        in_specs=cluster_specs(8 - EARLY) + [full(SUM)] * 3,
        out_specs=[full(SUM)] * 3,
        out_shape=[jax.ShapeDtypeStruct(SUM, F32)] * 3,
        cost_estimate=COST,
    )(*raws, *before)


def dot_wide(a, b):
    high = a.astype(BF)
    low = (a - high.astype(F32)).astype(BF)
    return dot(high, b) + dot(low, b)


def share_kernel(p_ref, d_ref, t_ref, *refs):
    means, out_ref = refs[:4], refs[4]
    mean = means[0][...].astype(F32)
    for part in means[1:]:
        mean += part[...].astype(F32)
    mean = (mean * (1.0 / CLUSTERS)).astype(BF)
    _, first = complex_square(mean[0:128, 0:128], mean[0:128, 128:256])
    _, second = complex_square(mean[128:256, 0:128], mean[128:256, 128:256])
    p = p_ref[...]
    g = dot_wide(p, first)
    share = t_ref[...] + 1.5 * g - 0.5 * dot_wide(p, second) + dot_wide(g - 0.5 * d_ref[...], first)
    out_ref[...] = (share * (1.0 / CLUSTERS)).astype(BF)


def consensus_kernel(s0, s1, s2, s3, out_ref, power_ref):
    even = s0[...].astype(F32) + s2[...].astype(F32)
    odd = s1[...].astype(F32) + s3[...].astype(F32)
    value = (even + odd).astype(BF)
    out_ref[...] = value
    kept = value.astype(F32)
    power = jnp.sum(kept * kept, axis=0, keepdims=True)
    power_ref[...] = power[:, 0:128] + power[:, 128:256]


def tail_kernel(value_ref, p0, p1, p2, p3, out_ref):
    power = (p0[...] + p2[...]) + (p1[...] + p3[...])
    row = lax.broadcasted_iota(jnp.int32, (8, 256), 0)
    tail = jnp.zeros((8, 256), F32)
    for k in range(3):
        term = power.astype(BF).astype(F32)
        power = power - term
        tail = jnp.where(row == k, jnp.concatenate([term, jnp.zeros_like(term)], axis=1), tail)
    out_ref[0:168, :] = value_ref[...]
    out_ref[168:176, :] = tail.astype(BF)


def finish_kernel(vectors, x_ref, pair_ref, c_ref, *refs):
    parts, out_ref, rows = refs[:8], refs[8], refs[9]
    x, pair, c = x_ref[0], pair_ref[0], c_ref[0]
    blocks = [
        side * 8 + lax.rem(x + X - d, X) * 2 + parity
        for side in (c, 1 - c)
        for d in range(X)
        for parity in (pair, 1 - pair)
    ]
    for k in range(16):
        tail = parts[k // 2][k % 2, 168:176, :].astype(F32)
        power = (tail[0:1, :] + tail[1:2, :]) + tail[2:3, :]
        rows[blocks[k]] = power[:, 0:128]
    power = rows[0]
    for k in range(1, 16):
        power += rows[k]
    factor = lax.rsqrt(power * (1.0 / vectors) + 1e-06)
    factor = jnp.concatenate([factor, factor], axis=1)
    for k in range(16):
        value = parts[k // 2][k % 2, 0:168, :].astype(F32) * factor
        out_ref[blocks[k]] = value.astype(BF)


def per_device(mantissas, exponents, channel, inverses):
    place_here = lax.axis_index("cluster")
    c = place_here % C
    x = place_here // C % X
    z = place_here // (C * X)
    mant, expo = mantissas[0], exponents.transpose(2, 0, 1)
    blocks, vectors, _ = mant.shape
    here = tuple(v.reshape(1).astype(jnp.int32) for v in (x, z % 2, c))
    sent = packed(
        *here, mant, expo, channel[0].reshape(blocks, 128, 128), inverses[0].reshape(blocks, 256, 128)
    )
    raws = [sent[0]]
    for k in range(1, 8):
        raws.append(moved(sent[k], pair_shifted(*SLOTS[k])))
    swapped = []
    for k in range(8):
        swapped.append(moved(raws[k], shifted(dc=1)))
    slots = [part for pair in zip(raws, swapped) for part in pair]
    before = early_sums(slots[: 2 * EARLY])
    means = mean_sums(slots[2 * EARLY :], before[3])
    means = [means, means, means, means]
    for d in (2, 1, 3):
        means[d] = moved(means[0], shifted(dz=2 * d))
    sums = late_sums(slots[2 * EARLY :], before[:3])
    share = whole(share_kernel, (*sums, *means), jax.ShapeDtypeStruct(SUM, BF))
    shares = [share, share, share, share]
    for d in (2, 1, 3):
        shares[d] = moved(share, shifted(dz=2 * d))
    value, power = whole(
        consensus_kernel, shares, (jax.ShapeDtypeStruct(SUM, BF), jax.ShapeDtypeStruct((1, 128), F32))
    )
    powers = [power, power, power, power]
    for d in (2, 1, 3):
        powers[d] = lax.ppermute(power, "sub", [(y, (y + d) % 4) for y in range(4)])
    mine = whole(tail_kernel, (value, *powers), jax.ShapeDtypeStruct((ROWS, 256), BF))
    both = jnp.stack([mine, moved(mine, pair_shifted(0, 1))])
    same = [both] + [moved(both, shifted(dx=d)) for d in (1, 2, 3)]
    other = [moved(part, shifted(dc=1)) for part in same]
    total = blocks * lax.axis_size("sub") * vectors
    return whole(
        lambda *refs: finish_kernel(total, *refs),
        (*here, *same, *other),
        jax.ShapeDtypeStruct((blocks, vectors, 256), BF),
        (pltpu.VMEM((16, 1, 128), F32),),
    )


def solution(mesh):
    placed = (
        P("cluster", "sub", None, None),
        P("cluster", "sub", None),
        P("cluster", "sub", None, None, None),
        P("cluster", "sub", None, None, None),
    )
    return jax.shard_map(
        per_device, mesh=mesh, in_specs=placed, out_specs=P("sub", None, None), check_vma=False
    )
```

```python
import jax
import jax.numpy as jnp
from jax import lax
from jax.experimental import pallas as pl
from jax.experimental.pallas import tpu as pltpu
from jax.sharding import PartitionSpec as P


Z, X, C = 8, 4, 2
CLUSTERS = Z * X * C
ROWS = 176
EARLY = 6
ROOM = 16 * 1024 * 1024
BF, F32 = jnp.bfloat16, jnp.float32


def place(z, x, c):
    return (z * X + x) * C + c


def shifted(dz=0, dx=0, dc=0):
    return [
        (place(z, x, c), place((z + dz) % Z, (x + dx) % X, c ^ dc))
        for z in range(Z)
        for x in range(X)
        for c in range(C)
    ]


def pair_shifted(dx, dp):
    return [
        (place(z, x, c), place(z ^ dp, (x + dx) % X, c))
        for z in range(Z)
        for x in range(X)
        for c in range(C)
    ]


SLOTS = ((0, 0), (1, 0), (3, 0), (0, 1), (2, 0), (1, 1), (3, 1), (2, 1))


def moved(value, pairs):
    return lax.ppermute(value, "cluster", pairs)


def dot(a, b):
    return jnp.dot(a, b, preferred_element_type=F32)


def complex_square(x, y):
    top = jnp.concatenate([x, y], axis=1)
    return top, jnp.concatenate([top, jnp.concatenate([-y, x], axis=1)], axis=0)


def pack_kernel(x_ref, pair_ref, c_ref, mant_ref, expo_ref, chan_ref, inv_ref, *outs):
    x, pair, c = x_ref[0], pair_ref[0], c_ref[0]
    row = lax.broadcasted_iota(jnp.int32, (168, 14), 0)
    first = lax.broadcasted_iota(jnp.int32, (168, 14), 1) * 12
    inside = ((row >= first) & (row < first + 12)).astype(F32).astype(BF)
    expo = jnp.concatenate([expo_ref[t] for t in range(14)], axis=0)
    scales = dot(inside, jnp.exp2(expo.astype(F32)).astype(BF))
    lane = lax.broadcasted_iota(jnp.int32, (168, 16), 1)
    for out, (dx, dp) in zip(outs, SLOTS):
        for k, side in enumerate((c, 1 - c)):
            r = side * 8 + lax.rem(x + dx, X) * 2 + (1 - pair if dp else pair)
            out[k, 0:256, :] = inv_ref[r]
            out[k, 256:384, :] = chan_ref[r]
            scale = jnp.sum(jnp.where(lane == r, scales, 0.0), axis=1, keepdims=True)
            out[k, 384:552, :] = (mant_ref[r].astype(F32) * scale).astype(BF)


def near(shape, dtype):
    return pltpu.VMEM(shape, dtype)


def whole(kernel, ins, outs, scratch=(), cost=None, fetched=False):
    vmem = pl.BlockSpec(memory_space=pltpu.VMEM)
    scalar = [value.shape == (1,) for value in ins]
    if not fetched:
        ins = [
            value if small else pltpu.with_memory_space_constraint(value, pltpu.VMEM)
            for value, small in zip(ins, scalar)
        ]
    return pl.pallas_call(
        kernel,
        in_specs=[pl.BlockSpec(memory_space=pltpu.SMEM) if small else vmem for small in scalar],
        out_specs=[vmem] * len(outs) if isinstance(outs, list) else vmem,
        out_shape=outs,
        scratch_shapes=scratch,
        cost_estimate=cost,
        compiler_params=pltpu.CompilerParams(vmem_limit_bytes=ROOM),
    )(*ins)


def packed(*ins):
    cost = pl.CostEstimate(flops=6000000, bytes_accessed=5000000, transcendentals=0)
    return whole(pack_kernel, ins, [near((2, 552, 128), BF)] * 8, cost=cost, fetched=True)


def square_of(raw):
    return complex_square(raw[0:128, :].T, raw[128:256, :].T)


def add_means(raws, av):
    for raw in raws:
        top, square = square_of(raw)
        av[0:128, :] += top.astype(F32)
        av[128:256, :] += dot(top, square)


def add_estimates(raws, p, d, t, av=None):
    sums = None
    for raw in raws:
        top, square = square_of(raw)
        cr, ci = raw[256:320, :], raw[320:384, :]
        match = jnp.concatenate(
            [jnp.concatenate([cr, -ci], axis=1), jnp.concatenate([ci, cr], axis=1)], axis=0
        )
        m = dot(raw[384:552, :], match).astype(BF)
        t1 = dot(m, square)
        t2 = dot(t1.astype(BF), square)
        t3 = dot(t2.astype(BF), square)
        new = (t1, t2, t3) + ((top.astype(F32), dot(top, square)) if av is not None else ())
        sums = new if sums is None else tuple(u + v for u, v in zip(sums, new))
    t1, t2, t3 = sums[:3]
    p[0:168, :] += t1
    d[0:168, :] += t2 - 2.0 * t1
    t[0:168, :] += 3.0 * t1 - 1.5 * t2 + 0.25 * t3
    if av is not None:
        av[0:128, :] += sums[3]
        av[128:256, :] += sums[4]


def early_kernel(*refs):
    raws, (p, d, t, av), held = refs[: 2 * EARLY], refs[2 * EARLY : -1], refs[-1]
    for k, raw in enumerate(raws):
        held[k] = raw[k % 2]
    for ref in (p, d, t, av):
        ref[...] = jnp.zeros_like(ref)

    def two(k, carry):
        add_estimates((held[2 * k], held[2 * k + 1]), p, d, t, av)
        return carry

    lax.fori_loop(0, EARLY, two, 0)


def mean_kernel(*refs):
    raws, before, out, av = refs[:-3], refs[-3], refs[-2], refs[-1]
    av[...] = before[...]
    add_means([raw[k % 2, 0:256, :] for k, raw in enumerate(raws)], av)
    ones = (
        lax.broadcasted_iota(jnp.int32, (128, 256), 0) == lax.broadcasted_iota(jnp.int32, (128, 256), 1)
    ).astype(F32) * 16.0
    first = av[0:128, :]
    out[0:128, :] = (first - ones).astype(BF)
    out[128:256, :] = (av[128:256, :] - 2.0 * first + ones).astype(BF)


def late_kernel(*refs):
    n = 2 * (8 - EARLY)
    raws, before, sums = refs[:n], refs[n : n + 3], refs[n + 3 :]
    for ref, old in zip(sums, before):
        ref[...] = old[...]
    for k in range(0, n, 2):
        add_estimates((raws[k][0], raws[k + 1][1]), *sums)


SUM = (168, 256)
SUMS = (SUM, SUM, SUM, (256, 256))
COST = pl.CostEstimate(flops=2000000000, bytes_accessed=3000000, transcendentals=0)


def early_sums(raws):
    scratch = [pltpu.VMEM((2 * EARLY, 552, 128), BF)]
    return whole(early_kernel, raws, [near(shape, F32) for shape in SUMS], scratch, COST)


def mean_sums(raws, before):
    scratch = [pltpu.VMEM((256, 256), F32)]
    return whole(mean_kernel, [*raws, before], near((256, 256), BF), scratch, COST)


def late_sums(raws, before):
    return whole(late_kernel, [*raws, *before], [near(SUM, F32)] * 3, cost=COST)


def dot_wide(a, b):
    high = a.astype(BF)
    low = (a - high.astype(F32)).astype(BF)
    return dot(high, b) + dot(low, b)


def share_kernel(p_ref, d_ref, t_ref, *refs):
    means, out_ref = refs[:4], refs[4]
    mean = means[0][...].astype(F32)
    for part in means[1:]:
        mean += part[...].astype(F32)
    mean = (mean * (1.0 / CLUSTERS)).astype(BF)
    _, first = complex_square(mean[0:128, 0:128], mean[0:128, 128:256])
    _, second = complex_square(mean[128:256, 0:128], mean[128:256, 128:256])
    p = p_ref[...]
    g = dot_wide(p, first)
    share = t_ref[...] + 1.5 * g - 0.5 * dot_wide(p, second) + dot_wide(g - 0.5 * d_ref[...], first)
    out_ref[...] = (share * (1.0 / CLUSTERS)).astype(BF)


def consensus_kernel(s0, s1, s2, s3, out_ref, power_ref):
    even = s0[...].astype(F32) + s2[...].astype(F32)
    odd = s1[...].astype(F32) + s3[...].astype(F32)
    value = (even + odd).astype(BF)
    out_ref[...] = value
    kept = value.astype(F32)
    power = jnp.sum(kept * kept, axis=0, keepdims=True)
    power_ref[...] = power[:, 0:128] + power[:, 128:256]


def tail_kernel(value_ref, p0, p1, p2, p3, out_ref):
    power = (p0[...] + p2[...]) + (p1[...] + p3[...])
    row = lax.broadcasted_iota(jnp.int32, (8, 256), 0)
    tail = jnp.zeros((8, 256), F32)
    for k in range(3):
        term = power.astype(BF).astype(F32)
        power = power - term
        tail = jnp.where(row == k, jnp.concatenate([term, jnp.zeros_like(term)], axis=1), tail)
    out_ref[0:168, :] = value_ref[...]
    out_ref[168:176, :] = tail.astype(BF)


def finish_kernel(vectors, x_ref, pair_ref, c_ref, *refs):
    parts, out_ref, rows = refs[:8], refs[8], refs[9]
    x, pair, c = x_ref[0], pair_ref[0], c_ref[0]
    blocks = [
        side * 8 + lax.rem(x + X - d, X) * 2 + parity
        for side in (c, 1 - c)
        for d in range(X)
        for parity in (pair, 1 - pair)
    ]
    for k in range(16):
        tail = parts[k // 2][k % 2, 168:176, :].astype(F32)
        power = (tail[0:1, :] + tail[1:2, :]) + tail[2:3, :]
        rows[blocks[k]] = power[:, 0:128]
    power = rows[0]
    for k in range(1, 16):
        power += rows[k]
    factor = lax.rsqrt(power * (1.0 / vectors) + 1e-06)
    factor = jnp.concatenate([factor, factor], axis=1)
    for k in range(16):
        value = parts[k // 2][k % 2, 0:168, :].astype(F32) * factor
        out_ref[blocks[k]] = value.astype(BF)


def per_device(mantissas, exponents, channel, inverses):
    place_here = lax.axis_index("cluster")
    c = place_here % C
    x = place_here // C % X
    z = place_here // (C * X)
    mant, expo = mantissas[0], exponents.transpose(2, 0, 1)
    blocks, vectors, _ = mant.shape
    here = tuple(v.reshape(1).astype(jnp.int32) for v in (x, z % 2, c))
    sent = packed(
        *here, mant, expo, channel[0].reshape(blocks, 128, 128), inverses[0].reshape(blocks, 256, 128)
    )
    raws = [sent[0]]
    for k in range(1, 8):
        raws.append(moved(sent[k], pair_shifted(*SLOTS[k])))
    swapped = []
    for k in range(8):
        swapped.append(moved(raws[k], shifted(dc=1)))
    slots = [part for pair in zip(raws, swapped) for part in pair]
    before = early_sums(slots[: 2 * EARLY])
    means = mean_sums(slots[2 * EARLY :], before[3])
    means = [means, means, means, means]
    for d in (2, 1, 3):
        means[d] = moved(means[0], shifted(dz=2 * d))
    sums = late_sums(slots[2 * EARLY :], before[:3])
    share = whole(share_kernel, (*sums, *means), near(SUM, BF))
    shares = [share, share, share, share]
    for d in (2, 1, 3):
        shares[d] = moved(share, shifted(dz=2 * d))
    value, power = whole(consensus_kernel, shares, [near(SUM, BF), near((1, 128), F32)])
    powers = [power, power, power, power]
    for d in (2, 1, 3):
        powers[d] = lax.ppermute(power, "sub", [(y, (y + d) % 4) for y in range(4)])
    mine = whole(tail_kernel, (value, *powers), near((ROWS, 256), BF))
    both = jnp.stack([mine, moved(mine, pair_shifted(0, 1))])
    same = [both] + [moved(both, shifted(dx=d)) for d in (1, 2, 3)]
    other = [moved(part, shifted(dc=1)) for part in same]
    total = blocks * lax.axis_size("sub") * vectors
    return whole(
        lambda *refs: finish_kernel(total, *refs),
        (*here, *same, *other),
        jax.ShapeDtypeStruct((blocks, vectors, 256), BF),
        (pltpu.VMEM((16, 1, 128), F32),),
    )


def solution(mesh):
    placed = (
        P("cluster", "sub", None, None),
        P("cluster", "sub", None),
        P("cluster", "sub", None, None, None),
        P("cluster", "sub", None, None, None),
    )
    return jax.shard_map(
        per_device, mesh=mesh, in_specs=placed, out_specs=P("sub", None, None), check_vma=False
    )
```

```python
import jax
import jax.numpy as jnp
from jax import lax
from jax.experimental import pallas as pl
from jax.experimental.pallas import tpu as pltpu
from jax.sharding import PartitionSpec as P


Z, X, C = 8, 4, 2
CLUSTERS = Z * X * C
ROWS = 176
EARLY = 6
ROOM = 16 * 1024 * 1024
BF, F32 = jnp.bfloat16, jnp.float32


def place(z, x, c):
    return (z * X + x) * C + c


def shifted(dz=0, dx=0, dc=0):
    return [
        (place(z, x, c), place((z + dz) % Z, (x + dx) % X, c ^ dc))
        for z in range(Z)
        for x in range(X)
        for c in range(C)
    ]


def pair_shifted(dx, dp):
    return [
        (place(z, x, c), place(z ^ dp, (x + dx) % X, c))
        for z in range(Z)
        for x in range(X)
        for c in range(C)
    ]


SLOTS = ((0, 0), (2, 1), (1, 0), (1, 1), (3, 0), (3, 1), (2, 0), (0, 1))


def ring_step(turn, count, spread):
    first = {k: (k ^ 1 if turn == 0 else (k - 1) % 4 if k % 2 == 0 else (k + 1) % 4) for k in range(4)}
    return [(spread(k, n), spread(first[k], n)) for k in range(4) for n in range(count)]


def on_z_ring(turn):
    return ring_step(turn, 2 * X * C, lambda q, n: place(2 * q + n // (X * C), n // C % X, n % C))


def on_sub_ring(turn):
    return ring_step(turn, 1, lambda y, n: y)


def moved(value, pairs):
    return lax.ppermute(value, "cluster", pairs)


def dot(a, b):
    return jnp.dot(a, b, preferred_element_type=F32)


def complex_square(x, y):
    top = jnp.concatenate([x, y], axis=1)
    return top, jnp.concatenate([top, jnp.concatenate([-y, x], axis=1)], axis=0)


def pack_kernel(x_ref, pair_ref, c_ref, *refs):
    far, outs, near, sems = refs[:4], refs[4:12], refs[12:16], refs[16]
    loads = [pltpu.make_async_copy(a, b, sems.at[k]) for k, (a, b) in enumerate(zip(far, near))]
    for load in loads:
        load.start()
    expo_ref, inv_ref, chan_ref, mant_ref = near
    x, pair, c = x_ref[0], pair_ref[0], c_ref[0]
    loads[0].wait()
    row = lax.broadcasted_iota(jnp.int32, (168, 14), 0)
    first = lax.broadcasted_iota(jnp.int32, (168, 14), 1) * 12
    inside = ((row >= first) & (row < first + 12)).astype(F32).astype(BF)
    expo = jnp.concatenate([expo_ref[t] for t in range(14)], axis=0)
    scales = dot(inside, jnp.exp2(expo.astype(F32)).astype(BF))
    lane = lax.broadcasted_iota(jnp.int32, (168, 16), 1)
    places = [
        (out, k, side * 8 + lax.rem(x + dx, X) * 2 + (1 - pair if dp else pair))
        for out, (dx, dp) in zip(outs, SLOTS)
        for k, side in enumerate((c, 1 - c))
    ]
    loads[1].wait()
    loads[2].wait()
    for out, k, r in places:
        out[k, 0:256, :] = inv_ref[r]
        out[k, 256:384, :] = chan_ref[r]
    loads[3].wait()
    for out, k, r in places:
        scale = jnp.sum(jnp.where(lane == r, scales, 0.0), axis=1, keepdims=True)
        out[k, 384:552, :] = (mant_ref[r].astype(F32) * scale).astype(BF)


def near(shape, dtype):
    return pltpu.VMEM(shape, dtype)


def whole(kernel, ins, outs, scratch=(), cost=None, space=pltpu.VMEM, out_space=pltpu.VMEM):
    vmem = pl.BlockSpec(memory_space=out_space)
    scalar = [value.shape == (1,) for value in ins]
    ins = [
        value if small else pltpu.with_memory_space_constraint(value, space)
        for value, small in zip(ins, scalar)
    ]
    return pl.pallas_call(
        kernel,
        in_specs=[pl.BlockSpec(memory_space=pltpu.SMEM if small else space) for small in scalar],
        out_specs=[vmem] * len(outs) if isinstance(outs, list) else vmem,
        out_shape=outs,
        scratch_shapes=scratch,
        cost_estimate=cost,
        compiler_params=pltpu.CompilerParams(vmem_limit_bytes=ROOM),
    )(*ins)


def packed(*ins):
    cost = pl.CostEstimate(flops=6000000, bytes_accessed=5000000, transcendentals=0)
    scratch = [pltpu.VMEM(value.shape, value.dtype) for value in ins[3:]] + [pltpu.SemaphoreType.DMA((4,))]
    return whole(pack_kernel, ins, [near((2, 552, 128), BF)] * 8, scratch, cost, pltpu.HBM)


def square_of(raw):
    return complex_square(raw[0:128, :].T, raw[128:256, :].T)


def add_means(raws, av):
    for raw in raws:
        top, square = square_of(raw)
        av[0:128, :] += top.astype(F32)
        av[128:256, :] += dot(top, square)


def add_estimates(raws, p, d, t, av=None):
    sums = None
    for raw in raws:
        top, square = square_of(raw)
        cr, ci = raw[256:320, :], raw[320:384, :]
        match = jnp.concatenate(
            [jnp.concatenate([cr, -ci], axis=1), jnp.concatenate([ci, cr], axis=1)], axis=0
        )
        m = dot(raw[384:552, :], match).astype(BF)
        t1 = dot(m, square)
        t2 = dot(t1.astype(BF), square)
        t3 = dot(t2.astype(BF), square)
        new = (t1, t2, t3) + ((top.astype(F32), dot(top, square)) if av is not None else ())
        sums = new if sums is None else tuple(u + v for u, v in zip(sums, new))
    t1, t2, t3 = sums[:3]
    p[0:168, :] += t1
    d[0:168, :] += t2 - 2.0 * t1
    t[0:168, :] += 3.0 * t1 - 1.5 * t2 + 0.25 * t3
    if av is not None:
        av[0:128, :] += sums[3]
        av[128:256, :] += sums[4]


def early_kernel(*refs):
    raws, (p, d, t, av), held = refs[: 2 * EARLY], refs[2 * EARLY : -1], refs[-1]
    for k, raw in enumerate(raws):
        held[k] = raw[k % 2]
    for ref in (p, d, t, av):
        ref[...] = jnp.zeros_like(ref)

    def two(k, carry):
        add_estimates((held[2 * k], held[2 * k + 1]), p, d, t, av)
        return carry

    lax.fori_loop(0, EARLY, two, 0)


def mean_kernel(*refs):
    raws, before, first_ref, second_ref, av = refs[:-4], *refs[-4:]
    av[...] = before[...]
    add_means([raw[k % 2, 0:256, :] for k, raw in enumerate(raws)], av)
    ones = (
        lax.broadcasted_iota(jnp.int32, (128, 256), 0) == lax.broadcasted_iota(jnp.int32, (128, 256), 1)
    ).astype(F32) * 16.0
    first = av[0:128, :]
    first_ref[...] = (first - ones).astype(BF)
    second_ref[...] = (av[128:256, :] - 2.0 * first + ones).astype(BF)


def pair_kernel(*refs):
    n = len(refs) // 3
    for a, b, out in zip(refs[:n], refs[n : 2 * n], refs[2 * n :]):
        out[...] = (a[...].astype(F32) + b[...].astype(F32)).astype(out.dtype)


def late_kernel(*refs):
    n = 2 * (8 - EARLY)
    raws, before, sums = refs[:n], refs[n : n + 3], refs[n + 3 :]
    for ref, old in zip(sums, before):
        ref[...] = old[...]
    for k in range(0, n, 2):
        add_estimates((raws[k][0], raws[k + 1][1]), *sums)


SUM = (168, 256)
SUMS = (SUM, SUM, SUM, (256, 256))
COST = pl.CostEstimate(flops=2000000000, bytes_accessed=3000000, transcendentals=0)


def early_sums(raws):
    scratch = [pltpu.VMEM((2 * EARLY, 552, 128), BF)]
    return whole(early_kernel, raws, [near(shape, F32) for shape in SUMS], scratch, COST)


def mean_sums(raws, before):
    scratch = [pltpu.VMEM((256, 256), F32)]
    return whole(mean_kernel, [*raws, before], [near((128, 256), BF)] * 2, scratch, COST)


def late_sums(raws, before):
    return whole(late_kernel, [*raws, *before], [near(SUM, F32)] * 3, cost=COST)


def dot_wide(a, b):
    high = a.astype(BF)
    low = (a - high.astype(F32)).astype(BF)
    return dot(high, b) + dot(low, b)


def share_kernel(p_ref, d_ref, t_ref, *refs):
    g0, g1, s0, s1, out_ref = refs
    first = ((g0[...].astype(F32) + g1[...].astype(F32)) * (1.0 / CLUSTERS)).astype(BF)
    second = ((s0[...].astype(F32) + s1[...].astype(F32)) * (1.0 / CLUSTERS)).astype(BF)
    _, first = complex_square(first[:, 0:128], first[:, 128:256])
    _, second = complex_square(second[:, 0:128], second[:, 128:256])
    p = p_ref[...]
    g = dot_wide(p, first)
    share = t_ref[...] + 1.5 * g - 0.5 * dot_wide(p, second) + dot_wide(g - 0.5 * d_ref[...], first)
    out_ref[...] = (share * (1.0 / CLUSTERS)).astype(BF)


def consensus_kernel(s0, s1, s2, s3, out_ref, power_ref):
    even = s0[...].astype(F32) + s2[...].astype(F32)
    odd = s1[...].astype(F32) + s3[...].astype(F32)
    value = (even + odd).astype(BF)
    out_ref[...] = value
    kept = value.astype(F32)
    power = jnp.sum(kept * kept, axis=0, keepdims=True)
    power_ref[...] = power[:, 0:128] + power[:, 128:256]


def tail_kernel(value_ref, p0, p1, out_ref):
    power = p0[...] + p1[...]
    row = lax.broadcasted_iota(jnp.int32, (8, 256), 0)
    tail = jnp.zeros((8, 256), F32)
    for k in range(3):
        term = power.astype(BF).astype(F32)
        power = power - term
        tail = jnp.where(row == k, jnp.concatenate([term, jnp.zeros_like(term)], axis=1), tail)
    out_ref[0:168, :] = value_ref[...]
    out_ref[168:176, :] = tail.astype(BF)


def finish_kernel(vectors, x_ref, pair_ref, c_ref, *refs):
    parts, out_ref, rows, held, sems = refs[:8], refs[8], refs[9], refs[10], refs[11]
    x, pair, c = x_ref[0], pair_ref[0], c_ref[0]
    blocks = [
        side * 8 + lax.rem(x + X - d, X) * 2 + parity
        for side in (c, 1 - c)
        for d in range(X)
        for parity in (pair, 1 - pair)
    ]
    for k in range(16):
        tail = parts[k // 2][k % 2, 168:176, :].astype(F32)
        power = (tail[0:1, :] + tail[1:2, :]) + tail[2:3, :]
        rows[blocks[k]] = power[:, 0:128]
    power = rows[0]
    for k in range(1, 16):
        power += rows[k]
    factor = lax.rsqrt(power * (1.0 / vectors) + 1e-06)
    factor = jnp.concatenate([factor, factor], axis=1)
    stores = []
    for k in range(16):
        value = parts[k // 2][k % 2, 0:168, :].astype(F32) * factor
        held[k] = value.astype(BF)
        stores.append(pltpu.make_async_copy(held.at[k], out_ref.at[blocks[k]], sems.at[k]))
        stores[k].start()
    for store in stores:
        store.wait()


def per_device(mantissas, exponents, channel, inverses):
    place_here = lax.axis_index("cluster")
    c = place_here % C
    x = place_here // C % X
    z = place_here // (C * X)
    mant, expo = mantissas[0], exponents.transpose(2, 0, 1)
    blocks, vectors, _ = mant.shape
    here = tuple(v.reshape(1).astype(jnp.int32) for v in (x, z % 2, c))
    sent = packed(
        *here, expo, inverses[0].reshape(blocks, 256, 128), channel[0].reshape(blocks, 128, 128), mant
    )
    raws = [sent[0]]
    for k in range(1, 8):
        raws.append(moved(sent[k], pair_shifted(*SLOTS[k])))
    swapped = []
    for k in range(8):
        swapped.append(moved(raws[k], shifted(dc=1)))
    slots = [part for pair in zip(raws, swapped) for part in pair]
    before = early_sums(slots[: 2 * EARLY])
    means = mean_sums(slots[2 * EARLY :], before[3])
    first = moved(means[0], on_z_ring(0))
    second = moved(means[1], on_z_ring(1))
    means = whole(pair_kernel, (*means, first, second), [near((128, 256), BF)] * 2)
    first = moved(means[0], on_z_ring(1))
    second = moved(means[1], on_z_ring(0))
    means = (means[0], first, means[1], second)
    sums = late_sums(slots[2 * EARLY :], before[:3])
    share = whole(share_kernel, (*sums, *means), near(SUM, BF))
    shares = [share, share, share, share]
    for d in (2, 1, 3):
        shares[d] = moved(share, shifted(dz=2 * d))
    value, power = whole(consensus_kernel, shares, [near(SUM, BF), near((1, 128), F32)])
    near_power = lax.ppermute(power, "sub", on_sub_ring(0))
    power = whole(pair_kernel, (power, near_power), near((1, 128), F32))
    far_power = lax.ppermute(power, "sub", on_sub_ring(1))
    mine = whole(tail_kernel, (value, power, far_power), near((ROWS, 256), BF))
    both = jnp.stack([mine, moved(mine, pair_shifted(0, 1))])
    same = [both] + [moved(both, shifted(dx=d)) for d in (1, 2, 3)]
    other = [moved(part, shifted(dc=1)) for part in same]
    total = blocks * lax.axis_size("sub") * vectors
    return whole(
        lambda *refs: finish_kernel(total, *refs),
        (*here, *same, *other),
        jax.ShapeDtypeStruct((blocks, vectors, 256), BF),
        (
            pltpu.VMEM((16, 1, 128), F32),
            pltpu.VMEM((16, vectors, 256), BF),
            pltpu.SemaphoreType.DMA((16,)),
        ),
        out_space=pltpu.HBM,
    )


def solution(mesh):
    placed = (
        P("cluster", "sub", None, None),
        P("cluster", "sub", None),
        P("cluster", "sub", None, None, None),
        P("cluster", "sub", None, None, None),
    )
    return jax.shard_map(
        per_device, mesh=mesh, in_specs=placed, out_specs=P("sub", None, None), check_vma=False
    )
```

```python
import jax
import jax.numpy as jnp
from jax import lax
from jax.experimental import pallas as pl
from jax.experimental.pallas import tpu as pltpu
from jax.sharding import PartitionSpec as P


Z, X, C = 8, 4, 2
CLUSTERS = Z * X * C
ROWS = 176
EARLY = 4
ROOM = 16 * 1024 * 1024
BF, F32 = jnp.bfloat16, jnp.float32


def place(z, x, c):
    return (z * X + x) * C + c


def shifted(dz=0, dx=0, dc=0):
    return [
        (place(z, x, c), place((z + dz) % Z, (x + dx) % X, c ^ dc))
        for z in range(Z)
        for x in range(X)
        for c in range(C)
    ]


def pair_shifted(dx, dp):
    return [
        (place(z, x, c), place(z ^ dp, (x + dx) % X, c))
        for z in range(Z)
        for x in range(X)
        for c in range(C)
    ]


SLOTS = ((0, 0), (1, 0), (3, 0), (0, 1), (2, 0), (1, 1), (3, 1), (2, 1))


def ring_step(turn, count, spread):
    first = {k: (k ^ 1 if turn == 0 else (k - 1) % 4 if k % 2 == 0 else (k + 1) % 4) for k in range(4)}
    return [(spread(k, n), spread(first[k], n)) for k in range(4) for n in range(count)]


def on_z_ring(turn):
    return ring_step(turn, 2 * X * C, lambda q, n: place(2 * q + n // (X * C), n // C % X, n % C))


def moved(value, pairs):
    return lax.ppermute(value, "cluster", pairs)


def dot(a, b):
    return jnp.dot(a, b, preferred_element_type=F32)


def complex_square(x, y):
    top = jnp.concatenate([x, y], axis=1)
    return top, jnp.concatenate([top, jnp.concatenate([-y, x], axis=1)], axis=0)


def pack_kernel(x_ref, pair_ref, c_ref, *refs):
    far, outs, near, sems = refs[:4], refs[4:12], refs[12:16], refs[16]
    loads = [pltpu.make_async_copy(a, b, sems.at[k]) for k, (a, b) in enumerate(zip(far, near))]
    for load in loads:
        load.start()
    expo_ref, inv_ref, chan_ref, mant_ref = near
    x, pair, c = x_ref[0], pair_ref[0], c_ref[0]
    loads[0].wait()
    row = lax.broadcasted_iota(jnp.int32, (168, 14), 0)
    first = lax.broadcasted_iota(jnp.int32, (168, 14), 1) * 12
    inside = ((row >= first) & (row < first + 12)).astype(F32).astype(BF)
    expo = jnp.concatenate([expo_ref[t] for t in range(14)], axis=0)
    scales = dot(inside, jnp.exp2(expo.astype(F32)).astype(BF))
    lane = lax.broadcasted_iota(jnp.int32, (168, 16), 1)
    places = [
        (out, k, side * 8 + lax.rem(x + dx, X) * 2 + (1 - pair if dp else pair))
        for out, (dx, dp) in zip(outs, SLOTS)
        for k, side in enumerate((c, 1 - c))
    ]
    loads[1].wait()
    loads[2].wait()
    for out, k, r in places:
        out[k, 0:256, :] = inv_ref[r]
        out[k, 256:384, :] = chan_ref[r]
    loads[3].wait()
    for out, k, r in places:
        scale = jnp.sum(jnp.where(lane == r, scales, 0.0), axis=1, keepdims=True)
        out[k, 384:552, :] = (mant_ref[r].astype(F32) * scale).astype(BF)


def near(shape, dtype):
    return pltpu.VMEM(shape, dtype)


def whole(kernel, ins, outs, scratch=(), cost=None, space=pltpu.VMEM, out_space=pltpu.VMEM):
    vmem = pl.BlockSpec(memory_space=out_space)
    scalar = [value.shape == (1,) for value in ins]
    ins = [
        value if small else pltpu.with_memory_space_constraint(value, space)
        for value, small in zip(ins, scalar)
    ]
    return pl.pallas_call(
        kernel,
        in_specs=[pl.BlockSpec(memory_space=pltpu.SMEM if small else space) for small in scalar],
        out_specs=[vmem] * len(outs) if isinstance(outs, list) else vmem,
        out_shape=outs,
        scratch_shapes=scratch,
        cost_estimate=cost,
        compiler_params=pltpu.CompilerParams(vmem_limit_bytes=ROOM),
    )(*ins)


def packed(*ins):
    cost = pl.CostEstimate(flops=6000000, bytes_accessed=5000000, transcendentals=0)
    scratch = [pltpu.VMEM(value.shape, value.dtype) for value in ins[3:]] + [pltpu.SemaphoreType.DMA((4,))]
    return whole(pack_kernel, ins, [near((2, 552, 128), BF)] * 8, scratch, cost, pltpu.HBM)


def square_of(raw):
    return complex_square(raw[0:128, :].T, raw[128:256, :].T)


def add_means(raws, av):
    for raw in raws:
        top, square = square_of(raw)
        av[0:128, :] += top.astype(F32)
        av[128:256, :] += dot(top, square)


def add_estimates(raws, p, d, t, av=None):
    sums = None
    for raw in raws:
        top, square = square_of(raw)
        cr, ci = raw[256:320, :], raw[320:384, :]
        match = jnp.concatenate(
            [jnp.concatenate([cr, -ci], axis=1), jnp.concatenate([ci, cr], axis=1)], axis=0
        )
        m = dot(raw[384:552, :], match).astype(BF)
        t1 = dot(m, square)
        t2 = dot(t1.astype(BF), square)
        t3 = dot(t2.astype(BF), square)
        new = (t1, t2, t3) + ((top.astype(F32), dot(top, square)) if av is not None else ())
        sums = new if sums is None else tuple(u + v for u, v in zip(sums, new))
    t1, t2, t3 = sums[:3]
    p[0:168, :] += t1
    d[0:168, :] += t2 - 2.0 * t1
    t[0:168, :] += 3.0 * t1 - 1.5 * t2 + 0.25 * t3
    if av is not None:
        av[0:128, :] += sums[3]
        av[128:256, :] += sums[4]


def early_kernel(*refs):
    raws, (p, d, t, av), held = refs[: 2 * EARLY], refs[2 * EARLY : -1], refs[-1]
    for k, raw in enumerate(raws):
        held[k] = raw[k % 2]
    for ref in (p, d, t, av):
        ref[...] = jnp.zeros_like(ref)

    def two(k, carry):
        add_estimates((held[2 * k], held[2 * k + 1]), p, d, t, av)
        return carry

    lax.fori_loop(0, EARLY, two, 0)


def mean_kernel(*refs):
    raws, before, first_ref, second_ref, av = refs[:-4], *refs[-4:]
    av[...] = before[...]
    add_means([raw[k % 2, 0:256, :] for k, raw in enumerate(raws)], av)
    ones = (
        lax.broadcasted_iota(jnp.int32, (128, 256), 0) == lax.broadcasted_iota(jnp.int32, (128, 256), 1)
    ).astype(F32) * 16.0
    first = av[0:128, :]
    first_ref[...] = (first - ones).astype(BF)
    second_ref[...] = (av[128:256, :] - 2.0 * first + ones).astype(BF)


def pair_kernel(*refs):
    n = len(refs) // 3
    for a, b, out in zip(refs[:n], refs[n : 2 * n], refs[2 * n :]):
        out[...] = (a[...].astype(F32) + b[...].astype(F32)).astype(out.dtype)


def late_kernel(*refs):
    n = 2 * (8 - EARLY)
    raws, before, sums = refs[:n], refs[n : n + 3], refs[n + 3 :]
    for ref, old in zip(sums, before):
        ref[...] = old[...]
    for k in range(0, n, 2):
        add_estimates((raws[k][0], raws[k + 1][1]), *sums)


SUM = (168, 256)
SUMS = (SUM, SUM, SUM, (256, 256))
COST = pl.CostEstimate(flops=2000000000, bytes_accessed=3000000, transcendentals=0)


def early_sums(raws):
    scratch = [pltpu.VMEM((2 * EARLY, 552, 128), BF)]
    return whole(early_kernel, raws, [near(shape, F32) for shape in SUMS], scratch, COST)


def mean_sums(raws, before):
    scratch = [pltpu.VMEM((256, 256), F32)]
    return whole(mean_kernel, [*raws, before], [near((128, 256), BF)] * 2, scratch, COST)


def late_sums(raws, before):
    return whole(late_kernel, [*raws, *before], [near(SUM, F32)] * 3, cost=COST)


def dot_wide(a, b):
    high = a.astype(BF)
    low = (a - high.astype(F32)).astype(BF)
    return dot(high, b) + dot(low, b)


def share_kernel(p_ref, d_ref, t_ref, *refs):
    g0, g1, s0, s1, out_ref = refs
    first = ((g0[...].astype(F32) + g1[...].astype(F32)) * (1.0 / CLUSTERS)).astype(BF)
    second = ((s0[...].astype(F32) + s1[...].astype(F32)) * (1.0 / CLUSTERS)).astype(BF)
    _, first = complex_square(first[:, 0:128], first[:, 128:256])
    _, second = complex_square(second[:, 0:128], second[:, 128:256])
    p = p_ref[...]
    g = dot_wide(p, first)
    share = t_ref[...] + 1.5 * g - 0.5 * dot_wide(p, second) + dot_wide(g - 0.5 * d_ref[...], first)
    out_ref[...] = (share * (1.0 / CLUSTERS)).astype(BF)


def consensus_kernel(s0, s1, s2, s3, out_ref, power_ref):
    even = s0[...].astype(F32) + s2[...].astype(F32)
    odd = s1[...].astype(F32) + s3[...].astype(F32)
    value = (even + odd).astype(BF)
    out_ref[...] = value
    kept = value.astype(F32)
    power = jnp.sum(kept * kept, axis=0, keepdims=True)
    power_ref[...] = power[:, 0:128] + power[:, 128:256]


def tail_kernel(value_ref, p0, p1, p2, p3, out_ref):
    power = (p0[...] + p2[...]) + (p1[...] + p3[...])
    row = lax.broadcasted_iota(jnp.int32, (8, 256), 0)
    tail = jnp.zeros((8, 256), F32)
    for k in range(3):
        term = power.astype(BF).astype(F32)
        power = power - term
        tail = jnp.where(row == k, jnp.concatenate([term, jnp.zeros_like(term)], axis=1), tail)
    out_ref[0:168, :] = value_ref[...]
    out_ref[168:176, :] = tail.astype(BF)


def finish_kernel(vectors, x_ref, pair_ref, c_ref, *refs):
    parts, (out_ref, rows, held, sems) = refs[:16], refs[16:]
    x, pair, c = x_ref[0], pair_ref[0], c_ref[0]
    order = [(0, pair), (0, 1 - pair)] + [(d, parity) for parity in (pair, 1 - pair) for d in (1, 3, 2)]
    blocks = [side * 8 + lax.rem(x + X - d, X) * 2 + parity for side in (c, 1 - c) for d, parity in order]
    for k in range(16):
        tail = parts[k][168:176, :].astype(F32)
        power = (tail[0:1, :] + tail[1:2, :]) + tail[2:3, :]
        rows[blocks[k]] = power[:, 0:128]
    power = rows[0]
    for k in range(1, 16):
        power += rows[k]
    factor = lax.rsqrt(power * (1.0 / vectors) + 1e-06)
    factor = jnp.concatenate([factor, factor], axis=1)
    stores = []
    for k in range(16):
        value = parts[k][0:168, :].astype(F32) * factor
        held[k] = value.astype(BF)
        stores.append(pltpu.make_async_copy(held.at[k], out_ref.at[blocks[k]], sems.at[k]))
        stores[k].start()
    for store in stores:
        store.wait()


def per_device(mantissas, exponents, channel, inverses):
    place_here = lax.axis_index("cluster")
    c = place_here % C
    x = place_here // C % X
    z = place_here // (C * X)
    mant, expo = mantissas[0], exponents.transpose(2, 0, 1)
    blocks, vectors, _ = mant.shape
    here = tuple(v.reshape(1).astype(jnp.int32) for v in (x, z % 2, c))
    sent = packed(
        *here, expo, inverses[0].reshape(blocks, 256, 128), channel[0].reshape(blocks, 128, 128), mant
    )
    raws = [sent[0]]
    for k in range(1, 8):
        raws.append(moved(sent[k], pair_shifted(*SLOTS[k])))
    swapped = []
    for k in range(8):
        swapped.append(moved(raws[k], shifted(dc=1)))
    slots = [part for pair in zip(raws, swapped) for part in pair]
    before = early_sums(slots[: 2 * EARLY])
    means = mean_sums(slots[2 * EARLY :], before[3])
    first = moved(means[0], on_z_ring(0))
    second = moved(means[1], on_z_ring(1))
    means = whole(pair_kernel, (*means, first, second), [near((128, 256), BF)] * 2)
    first = moved(means[0], on_z_ring(1))
    second = moved(means[1], on_z_ring(0))
    means = (means[0], first, means[1], second)
    sums = late_sums(slots[2 * EARLY :], before[:3])
    share = whole(share_kernel, (*sums, *means), near(SUM, BF))
    shares = [share, share, share, share]
    for d in (2, 1, 3):
        shares[d] = moved(share, shifted(dz=2 * d))
    value, power = whole(consensus_kernel, shares, [near(SUM, BF), near((1, 128), F32)])
    powers = [power, power, power, power]
    for d in (2, 1, 3):
        powers[d] = lax.ppermute(power, "sub", [(y, (y + d) % 4) for y in range(4)])
    mine = whole(tail_kernel, (value, *powers), near((ROWS, 256), BF))
    theirs = moved(mine, pair_shifted(0, 1))
    same = [mine, theirs]
    for value in (mine, theirs):
        for d in (1, 3, 2):
            same.append(moved(value, shifted(dx=d)))
    other = [moved(part, shifted(dc=1)) for part in same]
    total = blocks * lax.axis_size("sub") * vectors
    return whole(
        lambda *refs: finish_kernel(total, *refs),
        (*here, *same, *other),
        jax.ShapeDtypeStruct((blocks, vectors, 256), BF),
        (
            pltpu.VMEM((16, 1, 128), F32),
            pltpu.VMEM((16, vectors, 256), BF),
            pltpu.SemaphoreType.DMA((16,)),
        ),
        out_space=pltpu.HBM,
    )


def solution(mesh):
    placed = (
        P("cluster", "sub", None, None),
        P("cluster", "sub", None),
        P("cluster", "sub", None, None, None),
        P("cluster", "sub", None, None, None),
    )
    return jax.shard_map(
        per_device, mesh=mesh, in_specs=placed, out_specs=P("sub", None, None), check_vma=False
    )
```

```python
import jax
import jax.numpy as jnp
from jax import lax
from jax.experimental import pallas as pl
from jax.experimental.pallas import tpu as pltpu
from jax.sharding import PartitionSpec as P


Z, X, C = 8, 4, 2
CLUSTERS = Z * X * C
ROWS = 176
ROOM = 16 * 1024 * 1024
BF, F32 = jnp.bfloat16, jnp.float32


def place(z, x, c):
    return (z * X + x) * C + c


def shifted(dz=0, dx=0, dc=0):
    return [
        (place(z, x, c), place((z + dz) % Z, (x + dx) % X, c ^ dc))
        for z in range(Z)
        for x in range(X)
        for c in range(C)
    ]


def pair_shifted(dx, dp):
    return [
        (place(z, x, c), place(z ^ dp, (x + dx) % X, c))
        for z in range(Z)
        for x in range(X)
        for c in range(C)
    ]


SLOTS = ((0, 0), (1, 0), (3, 0), (0, 1), (2, 0), (1, 1), (3, 1), (2, 1))


def ring_step(turn, count, spread):
    first = {k: (k ^ 1 if turn == 0 else (k - 1) % 4 if k % 2 == 0 else (k + 1) % 4) for k in range(4)}
    return [(spread(k, n), spread(first[k], n)) for k in range(4) for n in range(count)]


def on_z_ring(turn):
    return ring_step(turn, 2 * X * C, lambda q, n: place(2 * q + n // (X * C), n // C % X, n % C))


def moved(value, pairs):
    return lax.ppermute(value, "cluster", pairs)


def dot(a, b):
    return jnp.dot(a, b, preferred_element_type=F32)


def complex_square(x, y):
    top = jnp.concatenate([x, y], axis=1)
    return top, jnp.concatenate([top, jnp.concatenate([-y, x], axis=1)], axis=0)


def pack_kernel(x_ref, pair_ref, c_ref, *refs):
    far, invs, sigs, near, sems = refs[:4], refs[4:12], refs[12:20], refs[20:24], refs[24]
    loads = [pltpu.make_async_copy(a, b, sems.at[k]) for k, (a, b) in enumerate(zip(far, near))]
    for load in loads:
        load.start()
    expo_ref, inv_ref, chan_ref, mant_ref = near
    x, pair, c = x_ref[0], pair_ref[0], c_ref[0]
    loads[0].wait()
    row = lax.broadcasted_iota(jnp.int32, (168, 14), 0)
    first = lax.broadcasted_iota(jnp.int32, (168, 14), 1) * 12
    inside = ((row >= first) & (row < first + 12)).astype(F32).astype(BF)
    expo = jnp.concatenate([expo_ref[t] for t in range(14)], axis=0)
    scales = dot(inside, jnp.exp2(expo.astype(F32)).astype(BF))
    lane = lax.broadcasted_iota(jnp.int32, (168, 16), 1)
    places = [
        (slot, k, side * 8 + lax.rem(x + dx, X) * 2 + (1 - pair if dp else pair))
        for slot, (dx, dp) in enumerate(SLOTS)
        for k, side in enumerate((c, 1 - c))
    ]
    loads[1].wait()
    for slot, k, r in places:
        invs[slot][k] = inv_ref[r]
    loads[2].wait()
    loads[3].wait()
    for slot, k, r in places:
        sigs[slot][k, 0:128, :] = chan_ref[r]
        scale = jnp.sum(jnp.where(lane == r, scales, 0.0), axis=1, keepdims=True)
        sigs[slot][k, 128:296, :] = (mant_ref[r].astype(F32) * scale).astype(BF)


def near(shape, dtype):
    return pltpu.VMEM(shape, dtype)


def whole(kernel, ins, outs, scratch=(), cost=None, space=pltpu.VMEM, out_space=pltpu.VMEM):
    vmem = pl.BlockSpec(memory_space=out_space)
    scalar = [value.shape == (1,) for value in ins]
    ins = [
        value if small else pltpu.with_memory_space_constraint(value, space)
        for value, small in zip(ins, scalar)
    ]
    return pl.pallas_call(
        kernel,
        in_specs=[pl.BlockSpec(memory_space=pltpu.SMEM if small else space) for small in scalar],
        out_specs=[vmem] * len(outs) if isinstance(outs, list) else vmem,
        out_shape=outs,
        scratch_shapes=scratch,
        cost_estimate=cost,
        compiler_params=pltpu.CompilerParams(vmem_limit_bytes=ROOM),
    )(*ins)


def packed(*ins):
    cost = pl.CostEstimate(flops=6000000, bytes_accessed=5000000, transcendentals=0)
    scratch = [pltpu.VMEM(value.shape, value.dtype) for value in ins[3:]] + [pltpu.SemaphoreType.DMA((4,))]
    outs = [near((2, 256, 128), BF)] * 8 + [near((2, 296, 128), BF)] * 8
    outs = whole(pack_kernel, ins, outs, scratch, cost, pltpu.HBM)
    return outs[:8], outs[8:]


def square_of(inv):
    return complex_square(inv[0:128, :].T, inv[128:256, :].T)


def add_estimates(invs, sigs, p, d, t):
    sums = None
    for inv, sig in zip(invs, sigs):
        _, square = square_of(inv)
        cr, ci = sig[0:64, :], sig[64:128, :]
        match = jnp.concatenate(
            [jnp.concatenate([cr, -ci], axis=1), jnp.concatenate([ci, cr], axis=1)], axis=0
        )
        m = dot(sig[128:296, :], match).astype(BF)
        t1 = dot(m, square)
        t2 = dot(t1.astype(BF), square)
        t3 = dot(t2.astype(BF), square)
        new = (t1, t2, t3)
        sums = new if sums is None else tuple(u + v for u, v in zip(sums, new))
    t1, t2, t3 = sums
    p[...] += t1
    d[...] += t2 - 2.0 * t1
    t[...] += 3.0 * t1 - 1.5 * t2 + 0.25 * t3


def estimate_kernel(before, *refs):
    invs, sigs, old, rest = refs[:8], refs[8:16], refs[16 : 16 + before], refs[16 + before :]
    p, d, t, held_inv, held_sig = rest
    for k in range(8):
        held_inv[k] = invs[k][k % 2]
        held_sig[k] = sigs[k][k % 2]
    for k, ref in enumerate((p, d, t)):
        ref[...] = old[k][...] if before else jnp.zeros_like(ref)

    def two(k, carry):
        k = 2 * k
        add_estimates((held_inv[k], held_inv[k + 1]), (held_sig[k], held_sig[k + 1]), p, d, t)
        return carry

    lax.fori_loop(0, 4, two, 0)


def mean_kernel(*refs):
    invs, first_ref, second_ref, av, held = refs[:-4], *refs[-4:]
    av[...] = jnp.zeros_like(av)
    for k, inv in enumerate(invs):
        held[k] = inv[k % 2]

    def four(k, carry):
        for j in range(4):
            top, square = square_of(held[4 * k + j])
            av[0:128, :] += top.astype(F32)
            av[128:256, :] += dot(top, square)
        return carry

    lax.fori_loop(0, 4, four, 0)
    ones = (
        lax.broadcasted_iota(jnp.int32, (128, 256), 0) == lax.broadcasted_iota(jnp.int32, (128, 256), 1)
    ).astype(F32) * 16.0
    first = av[0:128, :]
    first_ref[...] = (first - ones).astype(BF)
    second_ref[...] = (av[128:256, :] - 2.0 * first + ones).astype(BF)


def pair_kernel(*refs):
    n = len(refs) // 3
    for a, b, out in zip(refs[:n], refs[n : 2 * n], refs[2 * n :]):
        out[...] = (a[...].astype(F32) + b[...].astype(F32)).astype(out.dtype)


SUM = (168, 256)
COST = pl.CostEstimate(flops=2000000000, bytes_accessed=3000000, transcendentals=0)


def estimates(invs, sigs, before=()):
    scratch = [pltpu.VMEM((8, 256, 128), BF), pltpu.VMEM((8, 296, 128), BF)]
    return whole(
        lambda *refs: estimate_kernel(len(before), *refs),
        [*invs, *sigs, *before],
        [near(SUM, F32)] * 3,
        scratch,
        COST,
    )


def mean_sums(invs):
    scratch = [pltpu.VMEM((256, 256), F32), pltpu.VMEM((16, 256, 128), BF)]
    return whole(mean_kernel, invs, [near((128, 256), BF)] * 2, scratch, COST)


def dot_wide(a, b):
    high = a.astype(BF)
    low = (a - high.astype(F32)).astype(BF)
    return dot(high, b) + dot(low, b)


def share_kernel(p_ref, d_ref, t_ref, *refs):
    g0, g1, s0, s1, out_ref = refs
    first = ((g0[...].astype(F32) + g1[...].astype(F32)) * (1.0 / CLUSTERS)).astype(BF)
    second = ((s0[...].astype(F32) + s1[...].astype(F32)) * (1.0 / CLUSTERS)).astype(BF)
    _, first = complex_square(first[:, 0:128], first[:, 128:256])
    _, second = complex_square(second[:, 0:128], second[:, 128:256])
    p = p_ref[...]
    g = dot_wide(p, first)
    share = t_ref[...] + 1.5 * g - 0.5 * dot_wide(p, second) + dot_wide(g - 0.5 * d_ref[...], first)
    out_ref[...] = (share * (1.0 / CLUSTERS)).astype(BF)


def consensus_kernel(s0, s1, s2, s3, out_ref, power_ref):
    even = s0[...].astype(F32) + s2[...].astype(F32)
    odd = s1[...].astype(F32) + s3[...].astype(F32)
    value = (even + odd).astype(BF)
    out_ref[...] = value
    kept = value.astype(F32)
    power = jnp.sum(kept * kept, axis=0, keepdims=True)
    power_ref[...] = power[:, 0:128] + power[:, 128:256]


def tail_kernel(value_ref, p0, p1, p2, p3, out_ref):
    power = (p0[...] + p2[...]) + (p1[...] + p3[...])
    row = lax.broadcasted_iota(jnp.int32, (8, 256), 0)
    tail = jnp.zeros((8, 256), F32)
    for k in range(3):
        term = power.astype(BF).astype(F32)
        power = power - term
        tail = jnp.where(row == k, jnp.concatenate([term, jnp.zeros_like(term)], axis=1), tail)
    out_ref[0:168, :] = value_ref[...]
    out_ref[168:176, :] = tail.astype(BF)


def finish_kernel(vectors, x_ref, pair_ref, c_ref, *refs):
    parts, (out_ref, rows, held, sems) = refs[:16], refs[16:]
    x, pair, c = x_ref[0], pair_ref[0], c_ref[0]
    order = [(0, pair), (0, 1 - pair)] + [(d, parity) for parity in (pair, 1 - pair) for d in (1, 3, 2)]
    blocks = [side * 8 + lax.rem(x + X - d, X) * 2 + parity for side in (c, 1 - c) for d, parity in order]
    for k in range(16):
        tail = parts[k][168:176, :].astype(F32)
        power = (tail[0:1, :] + tail[1:2, :]) + tail[2:3, :]
        rows[blocks[k]] = power[:, 0:128]
    power = rows[0]
    for k in range(1, 16):
        power += rows[k]
    factor = lax.rsqrt(power * (1.0 / vectors) + 1e-06)
    factor = jnp.concatenate([factor, factor], axis=1)
    stores = []
    for k in range(16):
        value = parts[k][0:168, :].astype(F32) * factor
        held[k] = value.astype(BF)
        stores.append(pltpu.make_async_copy(held.at[k], out_ref.at[blocks[k]], sems.at[k]))
        stores[k].start()
    for store in stores:
        store.wait()


def per_device(mantissas, exponents, channel, inverses):
    place_here = lax.axis_index("cluster")
    c = place_here % C
    x = place_here // C % X
    z = place_here // (C * X)
    mant, expo = mantissas[0], exponents.transpose(2, 0, 1)
    blocks, vectors, _ = mant.shape
    here = tuple(v.reshape(1).astype(jnp.int32) for v in (x, z % 2, c))
    sent = packed(
        *here, expo, inverses[0].reshape(blocks, 256, 128), channel[0].reshape(blocks, 128, 128), mant
    )

    def regrouped(parts):
        raws, slots = [parts[0]], []
        for k in range(1, 8):
            raws.append(moved(parts[k], pair_shifted(*SLOTS[k])))
        for k in range(8):
            slots += [raws[k], moved(raws[k], shifted(dc=1))]
        return slots

    invs, sigs = regrouped(sent[0]), regrouped(sent[1])
    means = mean_sums(invs)
    first = moved(means[0], on_z_ring(0))
    second = moved(means[1], on_z_ring(1))
    sums = estimates(invs[:8], sigs[:8])
    means = whole(pair_kernel, (*means, first, second), [near((128, 256), BF)] * 2)
    first = moved(means[0], on_z_ring(1))
    second = moved(means[1], on_z_ring(0))
    means = (means[0], first, means[1], second)
    sums = estimates(invs[8:], sigs[8:], sums)
    share = whole(share_kernel, (*sums, *means), near(SUM, BF))
    shares = [share, share, share, share]
    for d in (2, 1, 3):
        shares[d] = moved(share, shifted(dz=2 * d))
    value, power = whole(consensus_kernel, shares, [near(SUM, BF), near((1, 128), F32)])
    powers = [power, power, power, power]
    for d in (2, 1, 3):
        powers[d] = lax.ppermute(power, "sub", [(y, (y + d) % 4) for y in range(4)])
    mine = whole(tail_kernel, (value, *powers), near((ROWS, 256), BF))
    theirs = moved(mine, pair_shifted(0, 1))
    same = [mine, theirs]
    for value in (mine, theirs):
        for d in (1, 3, 2):
            same.append(moved(value, shifted(dx=d)))
    other = [moved(part, shifted(dc=1)) for part in same]
    total = blocks * lax.axis_size("sub") * vectors
    return whole(
        lambda *refs: finish_kernel(total, *refs),
        (*here, *same, *other),
        jax.ShapeDtypeStruct((blocks, vectors, 256), BF),
        (
            pltpu.VMEM((16, 1, 128), F32),
            pltpu.VMEM((16, vectors, 256), BF),
            pltpu.SemaphoreType.DMA((16,)),
        ),
        out_space=pltpu.HBM,
    )


def solution(mesh):
    placed = (
        P("cluster", "sub", None, None),
        P("cluster", "sub", None),
        P("cluster", "sub", None, None, None),
        P("cluster", "sub", None, None, None),
    )
    return jax.shard_map(
        per_device, mesh=mesh, in_specs=placed, out_specs=P("sub", None, None), check_vma=False
    )
```

```python
import jax
import jax.numpy as jnp
from jax import lax
from jax.experimental import pallas as pl
from jax.experimental.pallas import tpu as pltpu
from jax.sharding import PartitionSpec as P


Z, X, C = 8, 4, 2
CLUSTERS = Z * X * C
ROWS = 176
ROOM = 16 * 1024 * 1024
BF, F32 = jnp.bfloat16, jnp.float32


def place(z, x, c):
    return (z * X + x) * C + c


def shifted(dz=0, dx=0, dc=0):
    return [
        (place(z, x, c), place((z + dz) % Z, (x + dx) % X, c ^ dc))
        for z in range(Z)
        for x in range(X)
        for c in range(C)
    ]


def pair_shifted(dx, dp):
    return [
        (place(z, x, c), place(z ^ dp, (x + dx) % X, c))
        for z in range(Z)
        for x in range(X)
        for c in range(C)
    ]


SLOTS = ((0, 0), (1, 0), (3, 0), (0, 1), (2, 0), (1, 1), (3, 1), (2, 1))


def core_shifted(shifts):
    return [
        (place(z, x, c), place(z ^ shifts[c][1], (x + shifts[c][0]) % X, c))
        for z in range(Z)
        for x in range(X)
        for c in range(C)
    ]


HALVES = (((1, 0), (3, 0)), ((0, 1), (2, 1)), ((1, 1), (2, 0)))
LAST = (3, 1)


def ring_step(turn, count, spread):
    first = {k: (k ^ 1 if turn == 0 else (k - 1) % 4 if k % 2 == 0 else (k + 1) % 4) for k in range(4)}
    return [(spread(k, n), spread(first[k], n)) for k in range(4) for n in range(count)]


def on_z_ring(turn):
    return ring_step(turn, 2 * X * C, lambda q, n: place(2 * q + n // (X * C), n // C % X, n % C))


def moved(value, pairs):
    return lax.ppermute(value, "cluster", pairs)


def dot(a, b):
    return jnp.dot(a, b, preferred_element_type=F32)


def complex_square(x, y):
    top = jnp.concatenate([x, y], axis=1)
    return top, jnp.concatenate([top, jnp.concatenate([-y, x], axis=1)], axis=0)


def pack_kernel(x_ref, pair_ref, c_ref, *refs):
    far, invs, sigs, near, sems = refs[:4], refs[4:12], refs[12:20], refs[20:24], refs[24]
    loads = [pltpu.make_async_copy(a, b, sems.at[k]) for k, (a, b) in enumerate(zip(far, near))]
    for load in loads:
        load.start()
    expo_ref, inv_ref, chan_ref, mant_ref = near
    x, pair, c = x_ref[0], pair_ref[0], c_ref[0]
    loads[0].wait()
    row = lax.broadcasted_iota(jnp.int32, (168, 14), 0)
    first = lax.broadcasted_iota(jnp.int32, (168, 14), 1) * 12
    inside = ((row >= first) & (row < first + 12)).astype(F32).astype(BF)
    expo = jnp.concatenate([expo_ref[t] for t in range(14)], axis=0)
    scales = dot(inside, jnp.exp2(expo.astype(F32)).astype(BF))
    lane = lax.broadcasted_iota(jnp.int32, (168, 16), 1)
    places = [
        (slot, k, side * 8 + lax.rem(x + dx, X) * 2 + (1 - pair if dp else pair))
        for slot, (dx, dp) in enumerate(SLOTS)
        for k, side in enumerate((c, 1 - c))
    ]
    loads[1].wait()
    for slot, k, r in places:
        invs[slot][k] = inv_ref[r]
    loads[2].wait()
    loads[3].wait()
    for slot, k, r in places:
        sigs[slot][k, 0:128, :] = chan_ref[r]
        scale = jnp.sum(jnp.where(lane == r, scales, 0.0), axis=1, keepdims=True)
        sigs[slot][k, 128:296, :] = (mant_ref[r].astype(F32) * scale).astype(BF)


def near(shape, dtype):
    return pltpu.VMEM(shape, dtype)


def whole(kernel, ins, outs, scratch=(), cost=None, space=pltpu.VMEM, out_space=pltpu.VMEM):
    vmem = pl.BlockSpec(memory_space=out_space)
    scalar = [value.shape == (1,) for value in ins]
    ins = [
        value if small else pltpu.with_memory_space_constraint(value, space)
        for value, small in zip(ins, scalar)
    ]
    return pl.pallas_call(
        kernel,
        in_specs=[pl.BlockSpec(memory_space=pltpu.SMEM if small else space) for small in scalar],
        out_specs=[vmem] * len(outs) if isinstance(outs, list) else vmem,
        out_shape=outs,
        scratch_shapes=scratch,
        cost_estimate=cost,
        compiler_params=pltpu.CompilerParams(vmem_limit_bytes=ROOM),
    )(*ins)


def packed(*ins):
    cost = pl.CostEstimate(flops=6000000, bytes_accessed=5000000, transcendentals=0)
    scratch = [pltpu.VMEM(value.shape, value.dtype) for value in ins[3:]] + [pltpu.SemaphoreType.DMA((4,))]
    outs = [near((2, 256, 128), BF)] * 8 + [near((2, 296, 128), BF)] * 8
    outs = whole(pack_kernel, ins, outs, scratch, cost, pltpu.HBM)
    return outs[:8], outs[8:]


def square_of(inv):
    return complex_square(inv[0:128, :].T, inv[128:256, :].T)


def add_estimates(invs, sigs, p, d, t):
    sums = None
    for inv, sig in zip(invs, sigs):
        _, square = square_of(inv)
        cr, ci = sig[0:64, :], sig[64:128, :]
        match = jnp.concatenate(
            [jnp.concatenate([cr, -ci], axis=1), jnp.concatenate([ci, cr], axis=1)], axis=0
        )
        m = dot(sig[128:296, :], match).astype(BF)
        t1 = dot(m, square)
        t2 = dot(t1.astype(BF), square)
        t3 = dot(t2.astype(BF), square)
        new = (t1, t2, t3)
        sums = new if sums is None else tuple(u + v for u, v in zip(sums, new))
    t1, t2, t3 = sums
    p[...] += t1
    d[...] += t2 - 2.0 * t1
    t[...] += 3.0 * t1 - 1.5 * t2 + 0.25 * t3


def estimate_kernel(before, *refs):
    invs, sigs, old, rest = refs[:8], refs[8:16], refs[16 : 16 + before], refs[16 + before :]
    p, d, t, held_inv, held_sig = rest
    for k in range(8):
        held_inv[k] = invs[k][k % 2]
        held_sig[k] = sigs[k][k % 2]
    for k, ref in enumerate((p, d, t)):
        ref[...] = old[k][...] if before else jnp.zeros_like(ref)

    def two(k, carry):
        k = 2 * k
        add_estimates((held_inv[k], held_inv[k + 1]), (held_sig[k], held_sig[k + 1]), p, d, t)
        return carry

    lax.fori_loop(0, 4, two, 0)


def mean_kernel(*refs):
    invs, first_ref, second_ref, av, held = refs[:-4], *refs[-4:]
    av[...] = jnp.zeros_like(av)
    for k, inv in enumerate(invs):
        held[k] = inv[k % 2]

    def four(k, carry):
        for j in range(4):
            top, square = square_of(held[4 * k + j])
            av[0:128, :] += top.astype(F32)
            av[128:256, :] += dot(top, square)
        return carry

    lax.fori_loop(0, 4, four, 0)
    ones = (
        lax.broadcasted_iota(jnp.int32, (128, 256), 0) == lax.broadcasted_iota(jnp.int32, (128, 256), 1)
    ).astype(F32) * 16.0
    first = av[0:128, :]
    first_ref[...] = (first - ones).astype(BF)
    second_ref[...] = (av[128:256, :] - 2.0 * first + ones).astype(BF)


def pair_kernel(*refs):
    n = len(refs) // 3
    for a, b, out in zip(refs[:n], refs[n : 2 * n], refs[2 * n :]):
        out[...] = (a[...].astype(F32) + b[...].astype(F32)).astype(out.dtype)


SUM = (168, 256)
COST = pl.CostEstimate(flops=2000000000, bytes_accessed=3000000, transcendentals=0)


def estimates(invs, sigs, before=()):
    scratch = [pltpu.VMEM((8, 256, 128), BF), pltpu.VMEM((8, 296, 128), BF)]
    return whole(
        lambda *refs: estimate_kernel(len(before), *refs),
        [*invs, *sigs, *before],
        [near(SUM, F32)] * 3,
        scratch,
        COST,
    )


def mean_sums(invs):
    scratch = [pltpu.VMEM((256, 256), F32), pltpu.VMEM((16, 256, 128), BF)]
    return whole(mean_kernel, invs, [near((128, 256), BF)] * 2, scratch, COST)


def dot_wide(a, b):
    high = a.astype(BF)
    low = (a - high.astype(F32)).astype(BF)
    return dot(high, b) + dot(low, b)


def share_kernel(p_ref, d_ref, t_ref, *refs):
    g0, g1, s0, s1, out_ref = refs
    first = ((g0[...].astype(F32) + g1[...].astype(F32)) * (1.0 / CLUSTERS)).astype(BF)
    second = ((s0[...].astype(F32) + s1[...].astype(F32)) * (1.0 / CLUSTERS)).astype(BF)
    _, first = complex_square(first[:, 0:128], first[:, 128:256])
    _, second = complex_square(second[:, 0:128], second[:, 128:256])
    p = p_ref[...]
    g = dot_wide(p, first)
    share = t_ref[...] + 1.5 * g - 0.5 * dot_wide(p, second) + dot_wide(g - 0.5 * d_ref[...], first)
    out_ref[...] = (share * (1.0 / CLUSTERS)).astype(BF)


def consensus_kernel(s0, s1, s2, s3, out_ref, power_ref):
    even = s0[...].astype(F32) + s2[...].astype(F32)
    odd = s1[...].astype(F32) + s3[...].astype(F32)
    value = (even + odd).astype(BF)
    out_ref[...] = value
    kept = value.astype(F32)
    power = jnp.sum(kept * kept, axis=0, keepdims=True)
    power_ref[...] = power[:, 0:128] + power[:, 128:256]


def tail_kernel(value_ref, other_ref, p0, p1, p2, p3, mine_ref, both_ref):
    power = (p0[...] + p2[...]) + (p1[...] + p3[...])
    row = lax.broadcasted_iota(jnp.int32, (8, 256), 0)
    tail = jnp.zeros((8, 256), F32)
    for k in range(3):
        term = power.astype(BF).astype(F32)
        power = power - term
        tail = jnp.where(row == k, jnp.concatenate([term, jnp.zeros_like(term)], axis=1), tail)
    tail = tail.astype(BF)
    mine_ref[0:168, :] = value_ref[...]
    mine_ref[168:176, :] = tail
    both_ref[0, 0:168, :] = value_ref[...]
    both_ref[0, 168:176, :] = tail
    both_ref[1, 0:168, :] = other_ref[...]
    both_ref[1, 168:176, :] = jnp.zeros_like(tail)


def finish_kernel(vectors, x_ref, pair_ref, c_ref, *refs):
    (both, *halves), (last, last_other), rest = refs[:7], refs[7:9], refs[9:]
    out_ref, rows, held, sems = rest
    x, pair, c = x_ref[0], pair_ref[0], c_ref[0]

    def chip(dx, dp):
        parity = pair + dp - 2 * pair * dp
        return lax.rem(x + X - dx, X) * 2 + parity

    parts, powers = [], []

    def add(ref, side, at, k=None):
        parts.append((ref if k is None else ref.at[k], side * 8 + at))

    for k in range(2):
        add(both, c if k == 0 else 1 - c, chip(0, 0), k)
    powers.append((both.at[0], chip(0, 0)))
    for n, half in enumerate(halves):
        side = c if n < 3 else 1 - c
        (a0, a1), (b0, b1) = HALVES[n % 3]
        at = chip(a0 + side * (b0 - a0), a1 + side * (b1 - a1))
        add(half, side, at, 0)
        add(half, 1 - side, at, 1)
        powers.append((half.at[0], at))
    add(last, c, chip(*LAST))
    add(last_other, 1 - c, chip(*LAST))
    powers.append((last, chip(*LAST)))
    for ref, at in powers:
        tail = ref[168:176, :].astype(F32)
        power = (tail[0:1, :] + tail[1:2, :]) + tail[2:3, :]
        rows[at] = power[:, 0:128]
    power = rows[0]
    for k in range(1, 8):
        power += rows[k]
    factor = lax.rsqrt(power * (1.0 / vectors) + 1e-06)
    factor = jnp.concatenate([factor, factor], axis=1)
    stores = []
    for k, (ref, at) in enumerate(parts):
        value = ref[0:168, :].astype(F32) * factor
        held[k] = value.astype(BF)
        stores.append(pltpu.make_async_copy(held.at[k], out_ref.at[at], sems.at[k]))
        stores[k].start()
    for store in stores:
        store.wait()


def per_device(mantissas, exponents, channel, inverses):
    place_here = lax.axis_index("cluster")
    c = place_here % C
    x = place_here // C % X
    z = place_here // (C * X)
    mant, expo = mantissas[0], exponents.transpose(2, 0, 1)
    blocks, vectors, _ = mant.shape
    here = tuple(v.reshape(1).astype(jnp.int32) for v in (x, z % 2, c))
    sent = packed(
        *here, expo, inverses[0].reshape(blocks, 256, 128), channel[0].reshape(blocks, 128, 128), mant
    )

    def regrouped(parts):
        raws, slots = [parts[0]], []
        for k in range(1, 8):
            raws.append(moved(parts[k], pair_shifted(*SLOTS[k])))
        for k in range(8):
            slots += [raws[k], moved(raws[k], shifted(dc=1))]
        return slots

    invs, sigs = regrouped(sent[0]), regrouped(sent[1])
    means = mean_sums(invs)
    first = moved(means[0], on_z_ring(0))
    second = moved(means[1], on_z_ring(1))
    sums = estimates(invs[:8], sigs[:8])
    means = whole(pair_kernel, (*means, first, second), [near((128, 256), BF)] * 2)
    first = moved(means[0], on_z_ring(1))
    second = moved(means[1], on_z_ring(0))
    means = (means[0], first, means[1], second)
    sums = estimates(invs[8:], sigs[8:], sums)
    share = whole(share_kernel, (*sums, *means), near(SUM, BF))
    shares = [share, share, share, share]
    for d in (2, 1, 3):
        shares[d] = moved(share, shifted(dz=2 * d))
    value, power = whole(consensus_kernel, shares, [near(SUM, BF), near((1, 128), F32)])
    other, other_power = moved(value, shifted(dc=1)), moved(power, shifted(dc=1))
    power = whole(pair_kernel, (power, other_power), near((1, 128), F32))
    powers = [power, power, power, power]
    for d in (2, 1, 3):
        powers[d] = lax.ppermute(power, "sub", [(y, (y + d) % 4) for y in range(4)])
    outs = [near((ROWS, 256), BF), near((2, ROWS, 256), BF)]
    mine, both = whole(tail_kernel, (value, other, *powers), outs)
    got = []
    for shifts in HALVES:
        got.append(moved(both, core_shifted(shifts)))
    last = moved(mine, pair_shifted(*LAST))
    got += [moved(part, shifted(dc=1)) for part in got]
    last_other = moved(last, shifted(dc=1))
    total = blocks * lax.axis_size("sub") * vectors
    return whole(
        lambda *refs: finish_kernel(total, *refs),
        (*here, both, *got, last, last_other),
        jax.ShapeDtypeStruct((blocks, vectors, 256), BF),
        (
            pltpu.VMEM((8, 1, 128), F32),
            pltpu.VMEM((16, vectors, 256), BF),
            pltpu.SemaphoreType.DMA((16,)),
        ),
        out_space=pltpu.HBM,
    )


def solution(mesh):
    placed = (
        P("cluster", "sub", None, None),
        P("cluster", "sub", None),
        P("cluster", "sub", None, None, None),
        P("cluster", "sub", None, None, None),
    )
    return jax.shard_map(
        per_device, mesh=mesh, in_specs=placed, out_specs=P("sub", None, None), check_vma=False
    )
```

```python
import jax
import jax.numpy as jnp
from jax import lax
from jax.experimental import pallas as pl
from jax.experimental.pallas import tpu as pltpu
from jax.sharding import PartitionSpec as P


Z, X, C = 8, 4, 2
CLUSTERS = Z * X * C
ROWS = 176
ROOM = 16 * 1024 * 1024
BF, F32 = jnp.bfloat16, jnp.float32


def place(z, x, c):
    return (z * X + x) * C + c


def shifted(dz=0, dx=0, dc=0):
    return [
        (place(z, x, c), place((z + dz) % Z, (x + dx) % X, c ^ dc))
        for z in range(Z)
        for x in range(X)
        for c in range(C)
    ]


def pair_shifted(dx, dp):
    return [
        (place(z, x, c), place(z ^ dp, (x + dx) % X, c))
        for z in range(Z)
        for x in range(X)
        for c in range(C)
    ]


def core_shifted(shifts):
    return [
        (place(z, x, c), place(z ^ shifts[c][1], (x + shifts[c][0]) % X, c))
        for z in range(Z)
        for x in range(X)
        for c in range(C)
    ]


HALVES = (((1, 0), (3, 0)), ((0, 1), (2, 1)), ((1, 1), (2, 0)))
LAST = (3, 1)


def ring_step(turn, count, spread):
    first = {k: (k ^ 1 if turn == 0 else (k - 1) % 4 if k % 2 == 0 else (k + 1) % 4) for k in range(4)}
    return [(spread(k, n), spread(first[k], n)) for k in range(4) for n in range(count)]


def on_z_ring(turn):
    return ring_step(turn, 2 * X * C, lambda q, n: place(2 * q + n // (X * C), n // C % X, n % C))


def moved(value, pairs):
    return lax.ppermute(value, "cluster", pairs)


def dot(a, b):
    return jnp.dot(a, b, preferred_element_type=F32)


def complex_square(x, y):
    top = jnp.concatenate([x, y], axis=1)
    return top, jnp.concatenate([top, jnp.concatenate([-y, x], axis=1)], axis=0)


def pack_kernel(x_ref, pair_ref, c_ref, *refs):
    far, invs, sigs, near, sems = refs[:4], refs[4:8], refs[8:12], refs[12:16], refs[16]
    loads = [pltpu.make_async_copy(a, b, sems.at[k]) for k, (a, b) in enumerate(zip(far, near))]
    for load in loads:
        load.start()
    expo_ref, inv_ref, chan_ref, mant_ref = near
    x, pair, c = x_ref[0], pair_ref[0], c_ref[0]
    loads[0].wait()
    row = lax.broadcasted_iota(jnp.int32, (168, 14), 0)
    first = lax.broadcasted_iota(jnp.int32, (168, 14), 1) * 12
    inside = ((row >= first) & (row < first + 12)).astype(F32).astype(BF)
    expo = jnp.concatenate([expo_ref[t] for t in range(14)], axis=0)
    scales = dot(inside, jnp.exp2(expo.astype(F32)).astype(BF))
    lane = lax.broadcasted_iota(jnp.int32, (168, 16), 1)

    def places(own, last, keep, give):
        chips = [(own, 0, 0), (last, *LAST)]
        for k, ((a0, a1), (b0, b1)) in enumerate(HALVES):
            for ref, side in ((keep, c), (give, 1 - c)):
                chips.append((ref.at[k], a0 + side * (b0 - a0), a1 + side * (b1 - a1)))
        for ref, dx, dp in chips:
            at = lax.rem(x + dx, X) * 2 + pair + dp - 2 * pair * dp
            for k, side in enumerate((c, 1 - c)):
                yield ref, k, side * 8 + at

    loads[1].wait()
    for ref, k, r in places(*invs):
        ref[k] = inv_ref[r]
    loads[2].wait()
    loads[3].wait()
    for ref, k, r in places(*sigs):
        ref[k, 0:128, :] = chan_ref[r]
        scale = jnp.sum(jnp.where(lane == r, scales, 0.0), axis=1, keepdims=True)
        ref[k, 128:296, :] = (mant_ref[r].astype(F32) * scale).astype(BF)


def near(shape, dtype):
    return pltpu.VMEM(shape, dtype)


def whole(kernel, ins, outs, scratch=(), cost=None, space=pltpu.VMEM, out_space=pltpu.VMEM):
    vmem = pl.BlockSpec(memory_space=out_space)
    scalar = [value.shape == (1,) for value in ins]
    ins = [
        value if small else pltpu.with_memory_space_constraint(value, space)
        for value, small in zip(ins, scalar)
    ]
    return pl.pallas_call(
        kernel,
        in_specs=[pl.BlockSpec(memory_space=pltpu.SMEM if small else space) for small in scalar],
        out_specs=[vmem] * len(outs) if isinstance(outs, list) else vmem,
        out_shape=outs,
        scratch_shapes=scratch,
        cost_estimate=cost,
        compiler_params=pltpu.CompilerParams(vmem_limit_bytes=ROOM),
    )(*ins)


def packed(*ins):
    cost = pl.CostEstimate(flops=6000000, bytes_accessed=5000000, transcendentals=0)
    scratch = [pltpu.VMEM(value.shape, value.dtype) for value in ins[3:]] + [pltpu.SemaphoreType.DMA((4,))]
    outs = [
        near((*lead, rows, 128), BF) for rows in (256, 296) for lead in ((2,), (2,), (3, 2), (3, 2))
    ]
    outs = whole(pack_kernel, ins, outs, scratch, cost, pltpu.HBM)
    return outs[:4], outs[4:]


def merge_kernel(keep_ref, got_ref, *outs):
    for k, out in enumerate(outs):
        out[0:2] = keep_ref[k]
        out[2:4] = got_ref[k]


def merged(keep, got):
    return whole(merge_kernel, (keep, got), [near((4, *keep.shape[2:]), BF)] * 3)


SINGLE = ((0,), (1,))
DOUBLE = ((0, 3), (1, 2))


def entries(refs):
    for k, ref in enumerate(refs):
        for at in (SINGLE if ref.shape[0] == 2 else DOUBLE)[k % 2]:
            yield ref[at]


def square_of(inv):
    return complex_square(inv[0:128, :].T, inv[128:256, :].T)


def add_estimates(invs, sigs, p, d, t):
    sums = None
    for inv, sig in zip(invs, sigs):
        _, square = square_of(inv)
        cr, ci = sig[0:64, :], sig[64:128, :]
        match = jnp.concatenate(
            [jnp.concatenate([cr, -ci], axis=1), jnp.concatenate([ci, cr], axis=1)], axis=0
        )
        m = dot(sig[128:296, :], match).astype(BF)
        t1 = dot(m, square)
        t2 = dot(t1.astype(BF), square)
        t3 = dot(t2.astype(BF), square)
        new = (t1, t2, t3)
        sums = new if sums is None else tuple(u + v for u, v in zip(sums, new))
    t1, t2, t3 = sums
    p[...] += t1
    d[...] += t2 - 2.0 * t1
    t[...] += 3.0 * t1 - 1.5 * t2 + 0.25 * t3


def estimate_kernel(before, *refs):
    *parts, p, d, t, held_inv, held_sig = refs
    parts, old = parts[: len(parts) - before], parts[len(parts) - before :]
    half = len(parts) // 2
    for k, (inv, sig) in enumerate(zip(entries(parts[:half]), entries(parts[half:]))):
        held_inv[k] = inv
        held_sig[k] = sig
    for k, ref in enumerate((p, d, t)):
        ref[...] = old[k][...] if before else jnp.zeros_like(ref)

    def two(k, carry):
        k = 2 * k
        add_estimates((held_inv[k], held_inv[k + 1]), (held_sig[k], held_sig[k + 1]), p, d, t)
        return carry

    lax.fori_loop(0, 4, two, 0)


def mean_kernel(*refs):
    invs, first_ref, second_ref, av, held = refs[:-4], *refs[-4:]
    av[...] = jnp.zeros_like(av)
    for k, inv in enumerate(entries(invs)):
        held[k] = inv

    def four(k, carry):
        for j in range(4):
            top, square = square_of(held[4 * k + j])
            av[0:128, :] += top.astype(F32)
            av[128:256, :] += dot(top, square)
        return carry

    lax.fori_loop(0, 4, four, 0)
    ones = (
        lax.broadcasted_iota(jnp.int32, (128, 256), 0) == lax.broadcasted_iota(jnp.int32, (128, 256), 1)
    ).astype(F32) * 16.0
    first = av[0:128, :]
    first_ref[...] = (first - ones).astype(BF)
    second_ref[...] = (av[128:256, :] - 2.0 * first + ones).astype(BF)


def pair_kernel(*refs):
    n = len(refs) // 3
    for a, b, out in zip(refs[:n], refs[n : 2 * n], refs[2 * n :]):
        out[...] = (a[...].astype(F32) + b[...].astype(F32)).astype(out.dtype)


SUM = (168, 256)
COST = pl.CostEstimate(flops=2000000000, bytes_accessed=3000000, transcendentals=0)


def estimates(invs, sigs, before=()):
    scratch = [pltpu.VMEM((8, 256, 128), BF), pltpu.VMEM((8, 296, 128), BF)]
    return whole(
        lambda *refs: estimate_kernel(len(before), *refs),
        [*invs, *sigs, *before],
        [near(SUM, F32)] * 3,
        scratch,
        COST,
    )


def mean_sums(invs):
    scratch = [pltpu.VMEM((256, 256), F32), pltpu.VMEM((16, 256, 128), BF)]
    return whole(mean_kernel, invs, [near((128, 256), BF)] * 2, scratch, COST)


def dot_wide(a, b):
    high = a.astype(BF)
    low = (a - high.astype(F32)).astype(BF)
    return dot(high, b) + dot(low, b)


def share_kernel(p_ref, d_ref, t_ref, *refs):
    g0, g1, s0, s1, out_ref = refs
    first = ((g0[...].astype(F32) + g1[...].astype(F32)) * (1.0 / CLUSTERS)).astype(BF)
    second = ((s0[...].astype(F32) + s1[...].astype(F32)) * (1.0 / CLUSTERS)).astype(BF)
    _, first = complex_square(first[:, 0:128], first[:, 128:256])
    _, second = complex_square(second[:, 0:128], second[:, 128:256])
    p = p_ref[...]
    g = dot_wide(p, first)
    share = t_ref[...] + 1.5 * g - 0.5 * dot_wide(p, second) + dot_wide(g - 0.5 * d_ref[...], first)
    out_ref[...] = (share * (1.0 / CLUSTERS)).astype(BF)


def consensus_kernel(s0, s1, s2, s3, out_ref, power_ref):
    even = s0[...].astype(F32) + s2[...].astype(F32)
    odd = s1[...].astype(F32) + s3[...].astype(F32)
    value = (even + odd).astype(BF)
    out_ref[...] = value
    kept = value.astype(F32)
    power = jnp.sum(kept * kept, axis=0, keepdims=True)
    power_ref[...] = power[:, 0:128] + power[:, 128:256]


def tail_kernel(value_ref, other_ref, p0, p1, p2, p3, mine_ref, both_ref):
    power = (p0[...] + p2[...]) + (p1[...] + p3[...])
    row = lax.broadcasted_iota(jnp.int32, (8, 256), 0)
    tail = jnp.zeros((8, 256), F32)
    for k in range(3):
        term = power.astype(BF).astype(F32)
        power = power - term
        tail = jnp.where(row == k, jnp.concatenate([term, jnp.zeros_like(term)], axis=1), tail)
    tail = tail.astype(BF)
    mine_ref[0:168, :] = value_ref[...]
    mine_ref[168:176, :] = tail
    both_ref[0, 0:168, :] = value_ref[...]
    both_ref[0, 168:176, :] = tail
    both_ref[1, 0:168, :] = other_ref[...]
    both_ref[1, 168:176, :] = jnp.zeros_like(tail)


def finish_kernel(vectors, x_ref, pair_ref, c_ref, *refs):
    (both, *halves), (last, last_other), rest = refs[:7], refs[7:9], refs[9:]
    out_ref, rows, held, sems = rest
    x, pair, c = x_ref[0], pair_ref[0], c_ref[0]

    def chip(dx, dp):
        parity = pair + dp - 2 * pair * dp
        return lax.rem(x + X - dx, X) * 2 + parity

    parts, powers = [], []

    def add(ref, side, at, k=None):
        parts.append((ref if k is None else ref.at[k], side * 8 + at))

    for k in range(2):
        add(both, c if k == 0 else 1 - c, chip(0, 0), k)
    powers.append((both.at[0], chip(0, 0)))
    for n, half in enumerate(halves):
        side = c if n < 3 else 1 - c
        (a0, a1), (b0, b1) = HALVES[n % 3]
        at = chip(a0 + side * (b0 - a0), a1 + side * (b1 - a1))
        add(half, side, at, 0)
        add(half, 1 - side, at, 1)
        powers.append((half.at[0], at))
    add(last, c, chip(*LAST))
    add(last_other, 1 - c, chip(*LAST))
    powers.append((last, chip(*LAST)))
    for ref, at in powers:
        tail = ref[168:176, :].astype(F32)
        power = (tail[0:1, :] + tail[1:2, :]) + tail[2:3, :]
        rows[at] = power[:, 0:128]
    power = rows[0]
    for k in range(1, 8):
        power += rows[k]
    factor = lax.rsqrt(power * (1.0 / vectors) + 1e-06)
    factor = jnp.concatenate([factor, factor], axis=1)
    stores = []
    for k, (ref, at) in enumerate(parts):
        value = ref[0:168, :].astype(F32) * factor
        held[k] = value.astype(BF)
        stores.append(pltpu.make_async_copy(held.at[k], out_ref.at[at], sems.at[k]))
        stores[k].start()
    for store in stores:
        store.wait()


def per_device(mantissas, exponents, channel, inverses):
    place_here = lax.axis_index("cluster")
    c = place_here % C
    x = place_here // C % X
    z = place_here // (C * X)
    mant, expo = mantissas[0], exponents.transpose(2, 0, 1)
    blocks, vectors, _ = mant.shape
    here = tuple(v.reshape(1).astype(jnp.int32) for v in (x, z % 2, c))
    sent = packed(
        *here, expo, inverses[0].reshape(blocks, 256, 128), channel[0].reshape(blocks, 128, 128), mant
    )

    def regrouped(parts):
        own, last, keep, give = parts
        last = moved(last, pair_shifted(*LAST))
        raws = [own, last]
        for k, part in enumerate(merged(keep, moved(give, shifted(dc=1)))):
            raws.append(moved(part, core_shifted(HALVES[k])))
        slots = []
        for raw in raws:
            slots += [raw, moved(raw, shifted(dc=1))]
        return slots

    invs, sigs = regrouped(sent[0]), regrouped(sent[1])
    means = mean_sums(invs)
    first = moved(means[0], on_z_ring(0))
    second = moved(means[1], on_z_ring(1))
    sums = estimates(invs[:6], sigs[:6])
    means = whole(pair_kernel, (*means, first, second), [near((128, 256), BF)] * 2)
    first = moved(means[0], on_z_ring(1))
    second = moved(means[1], on_z_ring(0))
    means = (means[0], first, means[1], second)
    sums = estimates(invs[6:], sigs[6:], sums)
    share = whole(share_kernel, (*sums, *means), near(SUM, BF))
    shares = [share, share, share, share]
    for d in (2, 1, 3):
        shares[d] = moved(share, shifted(dz=2 * d))
    value, power = whole(consensus_kernel, shares, [near(SUM, BF), near((1, 128), F32)])
    other, other_power = moved(value, shifted(dc=1)), moved(power, shifted(dc=1))
    power = whole(pair_kernel, (power, other_power), near((1, 128), F32))
    powers = [power, power, power, power]
    for d in (2, 1, 3):
        powers[d] = lax.ppermute(power, "sub", [(y, (y + d) % 4) for y in range(4)])
    outs = [near((ROWS, 256), BF), near((2, ROWS, 256), BF)]
    mine, both = whole(tail_kernel, (value, other, *powers), outs)
    got = []
    for shifts in HALVES:
        got.append(moved(both, core_shifted(shifts)))
    last = moved(mine, pair_shifted(*LAST))
    got += [moved(part, shifted(dc=1)) for part in got]
    last_other = moved(last, shifted(dc=1))
    total = blocks * lax.axis_size("sub") * vectors
    return whole(
        lambda *refs: finish_kernel(total, *refs),
        (*here, both, *got, last, last_other),
        jax.ShapeDtypeStruct((blocks, vectors, 256), BF),
        (
            pltpu.VMEM((8, 1, 128), F32),
            pltpu.VMEM((16, vectors, 256), BF),
            pltpu.SemaphoreType.DMA((16,)),
        ),
        out_space=pltpu.HBM,
    )


def solution(mesh):
    placed = (
        P("cluster", "sub", None, None),
        P("cluster", "sub", None),
        P("cluster", "sub", None, None, None),
        P("cluster", "sub", None, None, None),
    )
    return jax.shard_map(
        per_device, mesh=mesh, in_specs=placed, out_specs=P("sub", None, None), check_vma=False
    )
```

```python
import jax
import jax.numpy as jnp
from jax import lax
from jax.experimental import pallas as pl
from jax.experimental.pallas import tpu as pltpu
from jax.sharding import PartitionSpec as P


Z, X, C = 8, 4, 2
CLUSTERS = Z * X * C
ROWS = 176
ROOM = 16 * 1024 * 1024
BF, F32 = jnp.bfloat16, jnp.float32


def place(z, x, c):
    return (z * X + x) * C + c


def shifted(dz=0, dx=0, dc=0):
    return [
        (place(z, x, c), place((z + dz) % Z, (x + dx) % X, c ^ dc))
        for z in range(Z)
        for x in range(X)
        for c in range(C)
    ]


def pair_shifted(dx, dp):
    return [
        (place(z, x, c), place(z ^ dp, (x + dx) % X, c))
        for z in range(Z)
        for x in range(X)
        for c in range(C)
    ]


SLOTS = ((0, 0), (1, 0), (3, 0), (0, 1), (2, 0), (1, 1), (3, 1), (2, 1))


def core_shifted(shifts):
    return [
        (place(z, x, c), place(z ^ shifts[c][1], (x + shifts[c][0]) % X, c))
        for z in range(Z)
        for x in range(X)
        for c in range(C)
    ]


HALVES = (((1, 0), (3, 0)), ((0, 1), (2, 1)), ((1, 1), (2, 0)))
LAST = (3, 1)


def ring_step(turn, count, spread):
    first = {k: (k ^ 1 if turn == 0 else (k - 1) % 4 if k % 2 == 0 else (k + 1) % 4) for k in range(4)}
    return [(spread(k, n), spread(first[k], n)) for k in range(4) for n in range(count)]


def on_z_ring(turn):
    return ring_step(turn, 2 * X * C, lambda q, n: place(2 * q + n // (X * C), n // C % X, n % C))


def moved(value, pairs):
    return lax.ppermute(value, "cluster", pairs)


def dot(a, b):
    return jnp.dot(a, b, preferred_element_type=F32)


def complex_square(x, y):
    top = jnp.concatenate([x, y], axis=1)
    return top, jnp.concatenate([top, jnp.concatenate([-y, x], axis=1)], axis=0)


def pack_kernel(x_ref, pair_ref, c_ref, *refs):
    far, invs, sigs, near, sems = refs[:4], refs[4:12], refs[12:20], refs[20:24], refs[24]
    loads = [pltpu.make_async_copy(a, b, sems.at[k]) for k, (a, b) in enumerate(zip(far, near))]
    for load in loads:
        load.start()
    expo_ref, inv_ref, chan_ref, mant_ref = near
    x, pair, c = x_ref[0], pair_ref[0], c_ref[0]
    loads[0].wait()
    row = lax.broadcasted_iota(jnp.int32, (168, 14), 0)
    first = lax.broadcasted_iota(jnp.int32, (168, 14), 1) * 12
    inside = ((row >= first) & (row < first + 12)).astype(F32).astype(BF)
    expo = jnp.concatenate([expo_ref[t] for t in range(14)], axis=0)
    scales = dot(inside, jnp.exp2(expo.astype(F32)).astype(BF))
    lane = lax.broadcasted_iota(jnp.int32, (168, 16), 1)
    places = [
        (slot, k, side * 8 + lax.rem(x + dx, X) * 2 + (1 - pair if dp else pair))
        for slot, (dx, dp) in enumerate(SLOTS)
        for k, side in enumerate((c, 1 - c))
    ]
    loads[1].wait()
    for slot, k, r in places:
        invs[slot][k] = inv_ref[r]
    loads[2].wait()
    loads[3].wait()
    for slot, k, r in places:
        sigs[slot][k, 0:128, :] = chan_ref[r]
        scale = jnp.sum(jnp.where(lane == r, scales, 0.0), axis=1, keepdims=True)
        sigs[slot][k, 128:296, :] = (mant_ref[r].astype(F32) * scale).astype(BF)


def near(shape, dtype):
    return pltpu.VMEM(shape, dtype)


def whole(kernel, ins, outs, scratch=(), cost=None, space=pltpu.VMEM, out_space=pltpu.VMEM):
    vmem = pl.BlockSpec(memory_space=out_space)
    scalar = [value.shape == (1,) for value in ins]
    ins = [
        value if small else pltpu.with_memory_space_constraint(value, space)
        for value, small in zip(ins, scalar)
    ]
    return pl.pallas_call(
        kernel,
        in_specs=[pl.BlockSpec(memory_space=pltpu.SMEM if small else space) for small in scalar],
        out_specs=[vmem] * len(outs) if isinstance(outs, list) else vmem,
        out_shape=outs,
        scratch_shapes=scratch,
        cost_estimate=cost,
        compiler_params=pltpu.CompilerParams(vmem_limit_bytes=ROOM),
    )(*ins)


def packed(*ins):
    cost = pl.CostEstimate(flops=6000000, bytes_accessed=5000000, transcendentals=0)
    scratch = [pltpu.VMEM(value.shape, value.dtype) for value in ins[3:]] + [pltpu.SemaphoreType.DMA((4,))]
    outs = [near((2, 256, 128), BF)] * 8 + [near((2, 296, 128), BF)] * 8
    outs = whole(pack_kernel, ins, outs, scratch, cost, pltpu.HBM)
    return outs[:8], outs[8:]


def square_of(inv):
    return complex_square(inv[0:128, :].T, inv[128:256, :].T)


def add_estimates(invs, sigs, p, d, t):
    sums = None
    for inv, sig in zip(invs, sigs):
        _, square = square_of(inv)
        cr, ci = sig[0:64, :], sig[64:128, :]
        match = jnp.concatenate(
            [jnp.concatenate([cr, -ci], axis=1), jnp.concatenate([ci, cr], axis=1)], axis=0
        )
        m = dot(sig[128:296, :], match).astype(BF)
        t1 = dot(m, square)
        t2 = dot(t1.astype(BF), square)
        t3 = dot(t2.astype(BF), square)
        new = (t1, t2, t3)
        sums = new if sums is None else tuple(u + v for u, v in zip(sums, new))
    t1, t2, t3 = sums
    p[...] += t1
    d[...] += t2 - 2.0 * t1
    t[...] += 3.0 * t1 - 1.5 * t2 + 0.25 * t3


def estimate_kernel(before, *refs):
    invs, sigs, old, rest = refs[:8], refs[8:16], refs[16 : 16 + before], refs[16 + before :]
    p, d, t = rest
    for k, ref in enumerate((p, d, t)):
        ref[...] = old[k][...] if before else jnp.zeros_like(ref)
    for k in range(0, 8, 2):
        add_estimates((invs[k][0], invs[k + 1][1]), (sigs[k][0], sigs[k + 1][1]), p, d, t)


def mean_kernel(*refs):
    invs, first_ref, second_ref, av = refs[:-3], *refs[-3:]
    av[...] = jnp.zeros_like(av)
    for k, inv in enumerate(invs):
        top, square = square_of(inv[k % 2])
        av[0:128, :] += top.astype(F32)
        av[128:256, :] += dot(top, square)
    ones = (
        lax.broadcasted_iota(jnp.int32, (128, 256), 0) == lax.broadcasted_iota(jnp.int32, (128, 256), 1)
    ).astype(F32) * 16.0
    first = av[0:128, :]
    first_ref[...] = (first - ones).astype(BF)
    second_ref[...] = (av[128:256, :] - 2.0 * first + ones).astype(BF)


def pair_kernel(*refs):
    n = len(refs) // 3
    for a, b, out in zip(refs[:n], refs[n : 2 * n], refs[2 * n :]):
        out[...] = (a[...].astype(F32) + b[...].astype(F32)).astype(out.dtype)


SUM = (168, 256)
COST = pl.CostEstimate(flops=2000000000, bytes_accessed=3000000, transcendentals=0)


def estimates(invs, sigs, before=()):
    return whole(
        lambda *refs: estimate_kernel(len(before), *refs),
        [*invs, *sigs, *before],
        [near(SUM, F32)] * 3,
        cost=COST,
    )


def mean_sums(invs):
    scratch = [pltpu.VMEM((256, 256), F32)]
    return whole(mean_kernel, invs, [near((128, 256), BF)] * 2, scratch, COST)


def dot_wide(a, b):
    high = a.astype(BF)
    low = (a - high.astype(F32)).astype(BF)
    return dot(high, b) + dot(low, b)


def share_kernel(p_ref, d_ref, t_ref, *refs):
    g0, g1, s0, s1, out_ref = refs
    first = ((g0[...].astype(F32) + g1[...].astype(F32)) * (1.0 / CLUSTERS)).astype(BF)
    second = ((s0[...].astype(F32) + s1[...].astype(F32)) * (1.0 / CLUSTERS)).astype(BF)
    _, first = complex_square(first[:, 0:128], first[:, 128:256])
    _, second = complex_square(second[:, 0:128], second[:, 128:256])
    p = p_ref[...]
    g = dot_wide(p, first)
    share = t_ref[...] + 1.5 * g - 0.5 * dot_wide(p, second) + dot_wide(g - 0.5 * d_ref[...], first)
    out_ref[...] = (share * (1.0 / CLUSTERS)).astype(BF)


def consensus_kernel(s0, s1, s2, s3, out_ref, power_ref):
    even = s0[...].astype(F32) + s2[...].astype(F32)
    odd = s1[...].astype(F32) + s3[...].astype(F32)
    value = (even + odd).astype(BF)
    out_ref[...] = value
    kept = value.astype(F32)
    power = jnp.sum(kept * kept, axis=0, keepdims=True)
    power_ref[...] = power[:, 0:128] + power[:, 128:256]


def tail_kernel(value_ref, other_ref, p0, p1, p2, p3, mine_ref, both_ref):
    power = (p0[...] + p2[...]) + (p1[...] + p3[...])
    row = lax.broadcasted_iota(jnp.int32, (8, 256), 0)
    tail = jnp.zeros((8, 256), F32)
    for k in range(3):
        term = power.astype(BF).astype(F32)
        power = power - term
        tail = jnp.where(row == k, jnp.concatenate([term, jnp.zeros_like(term)], axis=1), tail)
    tail = tail.astype(BF)
    mine_ref[0:168, :] = value_ref[...]
    mine_ref[168:176, :] = tail
    both_ref[0, 0:168, :] = value_ref[...]
    both_ref[0, 168:176, :] = tail
    both_ref[1, 0:168, :] = other_ref[...]
    both_ref[1, 168:176, :] = jnp.zeros_like(tail)


def finish_kernel(vectors, x_ref, pair_ref, c_ref, *refs):
    (both, *halves), (last, last_other), rest = refs[:7], refs[7:9], refs[9:]
    out_ref, rows, held, sems = rest
    x, pair, c = x_ref[0], pair_ref[0], c_ref[0]

    def chip(dx, dp):
        parity = pair + dp - 2 * pair * dp
        return lax.rem(x + X - dx, X) * 2 + parity

    parts, powers = [], []

    def add(ref, side, at, k=None):
        parts.append((ref if k is None else ref.at[k], side * 8 + at))

    for k in range(2):
        add(both, c if k == 0 else 1 - c, chip(0, 0), k)
    powers.append((both.at[0], chip(0, 0)))
    for n, half in enumerate(halves):
        side = c if n < 3 else 1 - c
        (a0, a1), (b0, b1) = HALVES[n % 3]
        at = chip(a0 + side * (b0 - a0), a1 + side * (b1 - a1))
        add(half, side, at, 0)
        add(half, 1 - side, at, 1)
        powers.append((half.at[0], at))
    add(last, c, chip(*LAST))
    add(last_other, 1 - c, chip(*LAST))
    powers.append((last, chip(*LAST)))
    for ref, at in powers:
        tail = ref[168:176, :].astype(F32)
        power = (tail[0:1, :] + tail[1:2, :]) + tail[2:3, :]
        rows[at] = power[:, 0:128]
    power = rows[0]
    for k in range(1, 8):
        power += rows[k]
    factor = lax.rsqrt(power * (1.0 / vectors) + 1e-06)
    factor = jnp.concatenate([factor, factor], axis=1)
    stores = []
    for k, (ref, at) in enumerate(parts):
        value = ref[0:168, :].astype(F32) * factor
        held[k] = value.astype(BF)
        stores.append(pltpu.make_async_copy(held.at[k], out_ref.at[at], sems.at[k]))
        stores[k].start()
    for store in stores:
        store.wait()


def per_device(mantissas, exponents, channel, inverses):
    place_here = lax.axis_index("cluster")
    c = place_here % C
    x = place_here // C % X
    z = place_here // (C * X)
    mant, expo = mantissas[0], exponents.transpose(2, 0, 1)
    blocks, vectors, _ = mant.shape
    here = tuple(v.reshape(1).astype(jnp.int32) for v in (x, z % 2, c))
    sent = packed(
        *here, expo, inverses[0].reshape(blocks, 256, 128), channel[0].reshape(blocks, 128, 128), mant
    )

    def regrouped(parts):
        raws, slots = [parts[0]], []
        for k in range(1, 8):
            raws.append(moved(parts[k], pair_shifted(*SLOTS[k])))
        for k in range(8):
            slots += [raws[k], moved(raws[k], shifted(dc=1))]
        return slots

    invs, sigs = regrouped(sent[0]), regrouped(sent[1])
    means = mean_sums(invs)
    first = moved(means[0], on_z_ring(0))
    second = moved(means[1], on_z_ring(1))
    sums = estimates(invs[:8], sigs[:8])
    means = whole(pair_kernel, (*means, first, second), [near((128, 256), BF)] * 2)
    first = moved(means[0], on_z_ring(1))
    second = moved(means[1], on_z_ring(0))
    means = (means[0], first, means[1], second)
    sums = estimates(invs[8:], sigs[8:], sums)
    share = whole(share_kernel, (*sums, *means), near(SUM, BF))
    shares = [share, share, share, share]
    for d in (2, 1, 3):
        shares[d] = moved(share, shifted(dz=2 * d))
    value, power = whole(consensus_kernel, shares, [near(SUM, BF), near((1, 128), F32)])
    other, other_power = moved(value, shifted(dc=1)), moved(power, shifted(dc=1))
    power = whole(pair_kernel, (power, other_power), near((1, 128), F32))
    powers = [power, power, power, power]
    for d in (2, 1, 3):
        powers[d] = lax.ppermute(power, "sub", [(y, (y + d) % 4) for y in range(4)])
    outs = [near((ROWS, 256), BF), near((2, ROWS, 256), BF)]
    mine, both = whole(tail_kernel, (value, other, *powers), outs)
    got = []
    for shifts in HALVES:
        got.append(moved(both, core_shifted(shifts)))
    last = moved(mine, pair_shifted(*LAST))
    got += [moved(part, shifted(dc=1)) for part in got]
    last_other = moved(last, shifted(dc=1))
    total = blocks * lax.axis_size("sub") * vectors
    return whole(
        lambda *refs: finish_kernel(total, *refs),
        (*here, both, *got, last, last_other),
        jax.ShapeDtypeStruct((blocks, vectors, 256), BF),
        (
            pltpu.VMEM((8, 1, 128), F32),
            pltpu.VMEM((16, vectors, 256), BF),
            pltpu.SemaphoreType.DMA((16,)),
        ),
        out_space=pltpu.HBM,
    )


def solution(mesh):
    placed = (
        P("cluster", "sub", None, None),
        P("cluster", "sub", None),
        P("cluster", "sub", None, None, None),
        P("cluster", "sub", None, None, None),
    )
    return jax.shard_map(
        per_device, mesh=mesh, in_specs=placed, out_specs=P("sub", None, None), check_vma=False
    )
```
